256 devices in a mesh: side: 2 (over y_hi), grp: 64 (over z, y_lo, x), rep: 2 (over core).
Axes of the slice: x: 4, y: 4 (y_hi: 2, y_lo: 2; y = y_hi * 2 + y_lo), z: 8, core: 2. Of those that a mesh axis runs over, the one named last changes fastest.
Arguments:
- hidden_in: bfloat16 [64, 12288], replicated, may hold values from -6 to 6
- norm_gain: float32 [12288], replicated, may hold values from 0.2 to 1.8
- qkv_weight: bfloat16 [12288, 14336], P('side', ('grp', 'rep')), may hold values from -0.0546875 to 0.0546875
- out_weight: bfloat16 [12288, 12288], P(('grp', 'rep'), 'side'), may hold values from -0.21875 to 0.21875
- gate_weight: bfloat16 [12288, 17408], P('side', ('grp', 'rep')), may hold values from -0.0546875 to 0.0546875
- up_weight: bfloat16 [12288, 17408], P('side', ('grp', 'rep')), may hold values from -0.0546875 to 0.0546875
- down_weight: bfloat16 [17408, 12288], P(('grp', 'rep'), 'side'), may hold values from -0.1875 to 0.1875
- cache_keys: bfloat16 [512, 4096, 128], P(('side', 'grp', 'rep')), may hold values from -1500 to 1500, as said below
- cache_values: bfloat16 [512, 4096, 128], P(('side', 'grp', 'rep')), may hold values from -6 to 6
- positions: int32 [64], replicated, may hold values from 0 to 4095
- write_slots: int32 [64], replicated, may hold values from 0 to 4095
Outputs:
- mixed: bfloat16 [64, 12288], P(None, ('side', 'grp', 'rep'))
The draws below stay inside these ranges and needn't reach their ends.
Inputs may be any that keep to these rules, and one draw needn't show every extreme that they name: `cache_keys`: stored keys, already rotated at their own positions. `positions`: the row's cache holds position + 1 used slots, ending at its write slot.
All inputs are finite; a program needn't handle non-finite values.
Results may differ from the reference program's by a relative error of at most 0.012.
Values may be sent and summed in bfloat16 or wider, within the bound.
A program may use at most 64 MiB of HBM per device.

```python
import math
import jax
import jax.numpy as jnp
from jax import lax

D = 12288
H = 96
KVH = 8
HD = 128
WIN = 4096
FF = 17408
HPG = 12
MB = 32
ROWS = 64
N_SIDE = 2


def draw_cache_keys(key, part):
    sample_keys = jax.random.normal(jax.random.fold_in(key, 11), (KVH * ROWS, WIN, HD), jnp.float32)
    return jnp.clip(sample_keys, -1500.0, 1500.0).astype(jnp.bfloat16)


def plant(values, own_key, smallest, top_value):
    dims = values.shape
    spot = [jax.random.randint(jax.random.fold_in(own_key, axis), (), 0, dims[axis]) for axis in range(len(dims))]
    values = values.at[tuple(spot)].set(smallest)
    longest = dims.index(max(dims))
    spot[longest] = (spot[longest] + 1) % dims[longest]
    return values.at[tuple(spot)].set(top_value)


def spiked(values, key, source, target, parts, factor):
    owner, partner = [(jnp.arange(values.shape[dim]) // (values.shape[dim] // parts)).reshape([-1 if axis == dim else 1 for axis in range(values.ndim)]) for dim in (source, target)]
    chosen = jax.random.permutation(key, parts)[partner]
    strong = (owner == chosen) | (owner == (partner + parts // 2) % parts)
    return jnp.where(strong, factor * values, values)


def level_of(own_key, shape, pieces, low, high):
    def one(axis_at, shards_of):
        heights = jax.random.uniform(jax.random.fold_in(jax.random.fold_in(own_key, 6), axis_at), (shards_of,), jnp.float32, low / len(pieces), high / len(pieces))
        return jnp.repeat(jnp.exp(heights), shape[axis_at] // shards_of).reshape((-1,) + (1,) * (len(shape) - axis_at - 1))

    loudness = one(*pieces[0])
    for cut in pieces[1:]:
        loudness = loudness * one(*cut)
    return loudness


def gaussian(stream_key, dims, width, most, cuts=(), held_as=jnp.bfloat16):
    drawn = jax.random.normal(stream_key, dims, jnp.float32) * width
    if len(cuts) > 0:
        drawn = level_of(stream_key, dims, cuts, -0.22, 0.18) * drawn
    return jnp.clip(drawn, min=-most, max=most).astype(held_as)


def bell_draw_with(key, extent, width, reach, pieces, heavy, kind=jnp.bfloat16):
    result = width * jax.random.normal(key, extent, jnp.float32)
    if pieces:
        result = result * level_of(key, extent, pieces, -0.22, 0.18)
    return jnp.clip(spiked(result, jax.random.fold_in(key, 3), *heavy), -reach, reach).astype(kind)


def setup_inputs(seed: int = 0) -> dict:
    streams_of = jax.random.split(jax.random.key(seed), 12)
    hidden_in = gaussian(streams_of[0], (ROWS, D), 1.0, 6.0)
    norm_gain = jnp.clip(1.0 + 0.16 * jax.random.normal(streams_of[1], (D,), jnp.float32), 0.2, 1.8)
    qkv_weight = gaussian(streams_of[2], (D, KVH * (HPG + 2) * HD), D ** -0.5, 0.0546875, ((0, 2), (1, 128)))
    out_weight = bell_draw_with(streams_of[3], (H * HD, D), (H * HD) ** -0.5, 0.21875, ((0, 128), (1, 2)), (0, 1, 128, 5.5))
    gate_weight = gaussian(streams_of[4], (D, FF), D ** -0.5, 0.0546875, ((0, 2), (1, 128)))
    up_weight = gaussian(streams_of[5], (D, FF), D ** -0.5, 0.0546875, ((0, 2), (1, 128)))
    down_weight = bell_draw_with(streams_of[6], (FF, D), FF ** -0.5, 0.1875, ((0, 128), (1, 2)), (0, 1, 128, 5.5))
    cache_keys = draw_cache_keys(jax.random.fold_in(streams_of[11], 71), 0)
    cache_values = gaussian(streams_of[8], (KVH * ROWS, WIN, HD), 1.0, 6.0, ((0, 256),))
    positions = plant(jax.random.randint(streams_of[9], (ROWS,), 0, WIN), jax.random.fold_in(streams_of[9], 1), 0, WIN - 1).astype(jnp.int32)
    write_slots = plant(jax.random.randint(streams_of[10], (ROWS,), 0, WIN), jax.random.fold_in(streams_of[10], 1), 0, WIN - 1).astype(jnp.int32)
    return {"hidden_in": hidden_in, "norm_gain": norm_gain, "qkv_weight": qkv_weight, "out_weight": out_weight, "gate_weight": gate_weight, "up_weight": up_weight, "down_weight": down_weight, "cache_keys": cache_keys, "cache_values": cache_values, "positions": positions, "write_slots": write_slots}


EPSILON = 1e-05
THETA = 50000.0
MASKED = -1e+30

def normalize(rows_in, norm_gain):
    values = rows_in.astype(jnp.float32)
    center = lax.optimization_barrier(jnp.mean(values, axis=-1, keepdims=True))
    spread = lax.optimization_barrier(jnp.mean(jnp.square(values - center), axis=-1, keepdims=True))
    return ((values - center) * lax.rsqrt(spread + EPSILON) * norm_gain).astype(jnp.bfloat16)

def rotate(values, positions):
    half_width = values.shape[-1] // 2
    frequency = THETA ** (-2.0 * jnp.arange(half_width, dtype=jnp.float32) / values.shape[-1])
    angles = positions.astype(jnp.float32)[:, None] * frequency[None, :]
    cosine = jnp.cos(angles)[:, None, :]
    sine_part = jnp.sin(angles)[:, None, :]
    first_half = values[..., :half_width]
    second_half = values[..., half_width:]
    return jnp.concatenate([first_half * cosine - second_half * sine_part, second_half * cosine + first_half * sine_part], axis=-1)

def attend_one(inputs):
    query, keys, values, new_key, new_value, position, slot = inputs
    column = jnp.arange(keys.shape[0], dtype=jnp.int32)
    hit_slot = (column == slot)[:, None]
    keys_now = jnp.where(hit_slot, new_key[None, :], keys)
    values_now = jnp.where(hit_slot, new_value[None, :], values)
    scores = jnp.dot(query, keys_now.T, preferred_element_type=jnp.float32) * (1.0 / math.sqrt(query.shape[-1]))
    usable = (slot - column) % keys.shape[0] <= position
    scores = jnp.where(usable[None, :], scores, MASKED)
    highest = lax.optimization_barrier(jnp.max(scores, axis=-1, keepdims=True))
    weights = jnp.exp(scores - highest)
    probs = (weights / lax.optimization_barrier(jnp.sum(weights, axis=-1, keepdims=True))).astype(jnp.bfloat16)
    return jnp.dot(probs, values_now, preferred_element_type=jnp.float32).astype(jnp.bfloat16)

def per_entry(values):
    moved = values.reshape((N_SIDE, MB, KVH) + values.shape[2:])
    moved = jnp.swapaxes(moved, 1, 2)
    return moved.reshape((N_SIDE * KVH * MB,) + values.shape[2:])

def reference(hidden_in, norm_gain, qkv_weight, out_weight, gate_weight, up_weight, down_weight, cache_keys, cache_values, positions, write_slots):
    normed = normalize(hidden_in, norm_gain)
    projected = jnp.dot(normed, qkv_weight, preferred_element_type=jnp.float32).astype(jnp.bfloat16)
    projected = lax.optimization_barrier(projected).reshape(ROWS, HPG + 2, KVH, HD)
    projected = jnp.swapaxes(projected, 1, 2)
    queries = rotate(projected[:, :, :HPG].reshape(ROWS, H, HD).astype(jnp.float32), positions).astype(jnp.bfloat16)
    new_keys = rotate(projected[:, :, HPG].astype(jnp.float32), positions).astype(jnp.bfloat16)
    new_values = projected[:, :, HPG + 1]
    entry_queries = per_entry(queries.reshape(ROWS, KVH, HPG, HD))
    entry_keys = per_entry(new_keys)
    entry_values = per_entry(new_values)
    entry_positions = jnp.broadcast_to(positions.reshape(N_SIDE, 1, MB), (N_SIDE, KVH, MB)).reshape(-1)
    entry_slots = jnp.broadcast_to(write_slots.reshape(N_SIDE, 1, MB), (N_SIDE, KVH, MB)).reshape(-1)
    attended = lax.map(attend_one, (entry_queries, cache_keys, cache_values, entry_keys, entry_values, entry_positions, entry_slots))
    attended = jnp.swapaxes(attended.reshape(N_SIDE, KVH, MB, HPG * HD), 1, 2).reshape(ROWS, H * HD)
    from_heads = jnp.dot(attended, out_weight, preferred_element_type=jnp.float32)
    gate_sum = jnp.dot(normed, gate_weight, preferred_element_type=jnp.float32)
    up_sum = jnp.dot(normed, up_weight, preferred_element_type=jnp.float32)
    activated = (jax.nn.silu(gate_sum) * up_sum).astype(jnp.bfloat16)
    from_units = jnp.dot(activated, down_weight, preferred_element_type=jnp.float32)
    return (hidden_in.astype(jnp.float32) + from_heads + from_units).astype(jnp.bfloat16)
```

```python
import math

import jax
import jax.numpy as jnp
import numpy as np
from jax import lax
from jax.experimental import pallas as pl
from jax.experimental.pallas import tpu as pltpu
from jax.sharding import PartitionSpec as P

MESH = pl.DeviceIdType.MESH
D = 12288
HALF = 6144
EPSILON = 1e-05
THETA = 50000.0
MASKED = -1e30
WIN = 4096
HD = 128
COLS = 112
FFB = 136
OB = 96
NCOL = 3072
SCALE = 1.0 / math.sqrt(HD)
F32 = jnp.float32
BF16 = jnp.bfloat16
NT = (((1,), (1,)), ((), ()))
TN = (((0,), (0,)), ((), ()))


def kernel(
    hidden, gain, qkv, out_w, gate, up, down, keys, values, pos, slots, freq, out,
    hid_v, gain_v, qkv_v, wo_v, gate_v, up_v, wd_v, k_v, v_v, normed_v,
    send1, recv1, qrow, cs_v, att_v, recv2, lhs_v, gu_send, gu_recv, act_v, acc_v,
    p1send, recvp1, p2send, recvp2, res_v,
    load_sem, s1, r1, spre, rpre, s2, r2, s3, r3, s4, r4, sp1, rp1, sp2, rp2,
):
    s = lax.axis_index("side")
    g = lax.axis_index("grp")
    c = lax.axis_index("rep")
    z = g // 8
    chip = g % 8
    j = 2 * g + c
    d16 = 2 * chip + c
    row_off = 64 * (chip % 2)

    def load(src, dst, n):
        cp = pltpu.make_async_copy(src, dst, load_sem.at[n])
        cp.start()
        return cp

    hid_cp = load(hidden, hid_v, 0)
    gain_cp = load(gain, gain_v, 1)
    qkv_cp = load(qkv, qkv_v.at[pl.ds(0, COLS)], 2)
    gate_cp = load(gate, gate_v, 3)
    up_cp = load(up, up_v, 4)
    k_cp = load(keys, k_v, 5)
    v_cp = load(values, v_v, 6)
    own_cols = pl.ds(pl.multiple_of(NCOL * c, NCOL), NCOL)
    wo_cp = load(
        out_w.at[:, own_cols], wo_v.at[pl.ds(pl.multiple_of(row_off + OB * c, 32), OB)], 7
    )
    wd_cp = load(down.at[:, own_cols], wd_v.at[c], 8)

    barrier = pltpu.get_barrier_semaphore()

    def greet(n, carry):
        b, rest = n // 128, n % 128

        @pl.when(jnp.logical_not((b == s) & (rest == j)))
        def _():
            pl.semaphore_signal(
                barrier, inc=1, device_id=(b, rest // 2, rest % 2), device_id_type=MESH
            )

        return carry

    lax.fori_loop(0, 256, greet, 0)

    qkv_v[pl.ds(COLS, 16), :] = jnp.zeros((16, HALF), BF16)
    wo_v[pl.ds(pl.multiple_of(192 - 192 * (chip % 2), 64), 64), :] = jnp.zeros((64, NCOL), BF16)

    hid_cp.wait()

    def chunk(i):
        return hid_v[:, pl.ds(pl.multiple_of(i * 128, 128), 128)].astype(F32)

    total = lax.fori_loop(
        0, 96, lambda i, a: a + chunk(i), jnp.zeros((64, 128), F32), unroll=8
    )
    mean = jnp.sum(total, axis=1, keepdims=True) * (1.0 / D)

    def square(i, a):
        d = chunk(i) - mean
        return a + d * d

    spread = lax.fori_loop(0, 96, square, jnp.zeros((64, 128), F32), unroll=8)
    var = jnp.sum(spread, axis=1, keepdims=True) * (1.0 / D)
    rstd = lax.rsqrt(var + EPSILON)
    gain_cp.wait()

    def norm(i, carry):
        n = s * 48 + i
        v = (chunk(n) - mean) * rstd * gain_v[pl.ds(n, 1), :]
        normed_v[:, pl.ds(pl.multiple_of(i * 128, 128), 128)] = v.astype(BF16)
        return carry

    lax.fori_loop(0, 48, norm, 0, unroll=4)

    qkv_cp.wait()
    term = lax.dot_general(normed_v[...], qkv_v[...], NT, preferred_element_type=F32)
    m, t = j // 8, j % 8
    rolled = pltpu.roll(term, (128 - 16 * t) % 128, 1)
    lane = lax.broadcasted_iota(jnp.int32, (64, 128), 1)
    first = jnp.where(lane < COLS - 16 * t, rolled, 0.0)
    second = jnp.where(lane >= 128 - 16 * t, rolled, 0.0)
    for n in range(32):
        send1[n] = first[2 * n : 2 * n + 2]
        send1[32 + n] = second[2 * n : 2 * n + 2]

    pl.semaphore_wait(barrier, 255)

    valid = (t <= 6, t >= 1)
    for piece in range(2):
        q = jnp.maximum(7 * m + t - piece, 0)
        k, cc = q % 8, q // 8
        slot = jnp.minimum(cc, 13) * 4 + piece * 2 + s

        @pl.when(valid[piece])
        def _():
            def push(n, carry):
                b, i = n // 16, n % 16
                there = 8 * k + i // 2

                @pl.when(jnp.logical_not((b == s) & (there == g) & (i % 2 == c)))
                def _():
                    pltpu.make_async_remote_copy(
                        src_ref=send1.at[32 * piece + n],
                        dst_ref=recv1.at[slot],
                        send_sem=s1,
                        recv_sem=r1,
                        device_id=(b, there, i % 2),
                        device_id_type=MESH,
                    ).start()

                return carry

            lax.fori_loop(0, 32, push, 0)

            @pl.when(k == z)
            def _():
                recv1[slot] = send1[32 * piece + s * 16 + d16]

    other_cols = pl.ds(pl.multiple_of(NCOL * (1 - c), NCOL), NCOL)
    sibling = (s, g, 1 - c)
    pre_out = pltpu.make_async_remote_copy(
        src_ref=out_w.at[:, other_cols],
        dst_ref=wo_v.at[pl.ds(pl.multiple_of(row_off + OB * c, 32), OB)],
        send_sem=spre.at[0],
        recv_sem=rpre.at[0],
        device_id=sibling,
        device_id_type=MESH,
    )
    pre_out.start()
    pre_down = pltpu.make_async_remote_copy(
        src_ref=down.at[:, other_cols],
        dst_ref=wd_v.at[c],
        send_sem=spre.at[1],
        recv_sem=rpre.at[1],
        device_id=sibling,
        device_id_type=MESH,
    )
    pre_down.start()

    gate_cp.wait()
    gu_send[:, 0:64] = lax.dot_general(
        gate_v[...], normed_v[...], NT, preferred_element_type=F32
    )
    up_cp.wait()
    gu_send[:, 64:128] = lax.dot_general(
        up_v[...], normed_v[...], NT, preferred_element_type=F32
    )
    gu = pltpu.make_async_remote_copy(
        src_ref=gu_send,
        dst_ref=gu_recv,
        send_sem=s3,
        recv_sem=r3,
        device_id=(1 - s, g, c),
        device_id_type=MESH,
    )
    gu.start()

    col0 = 48 * (128 * s + j)
    tile = jnp.minimum(col0 // 128, 94)
    res_v[...] = hid_v[:, pl.ds(pl.multiple_of(tile * 128, 128), 256)].astype(F32).T
    res_off = pl.multiple_of(col0 - tile * 128, 16)

    lane1 = lax.broadcasted_iota(jnp.int32, (1, 128), 1)
    row0 = 32 * s + 2 * d16
    for r in range(2):
        angle = pos[row0 + r].astype(F32) * freq[...]
        sine = jnp.sin(angle)
        cs_v[2 * r : 2 * r + 1, :] = jnp.cos(angle)
        cs_v[2 * r + 1 : 2 * r + 2, :] = jnp.where(lane1 < 64, -sine, sine)
    qrow[...] = jnp.zeros((2, 16, 128), F32)

    mine = ((t <= 6) & ((7 * m + t) % 8 == z)) | ((t >= 1) & ((7 * m + t + 7) % 8 == z))

    def wait_recv(src, dst, send, recv):
        pltpu.make_async_remote_copy(
            src_ref=src, dst_ref=dst, send_sem=send, recv_sem=recv,
            device_id=sibling, device_id_type=MESH,
        ).wait_recv()

    def wait_send(src, dst, send, recv):
        pltpu.make_async_remote_copy(
            src_ref=src, dst_ref=dst, send_sem=send, recv_sem=recv,
            device_id=sibling, device_id_type=MESH,
        ).wait_send()

    @pl.when(mine)
    def _():
        part = recv1.at[pl.ds(0, 55)]
        wait_recv(part, part, s1, r1)

    @pl.when(jnp.logical_not(mine))
    def _():
        wait_recv(recv1, recv1, s1, r1)

    for cc in range(14):
        both = (recv1[4 * cc] + recv1[4 * cc + 1]) + (recv1[4 * cc + 2] + recv1[4 * cc + 3])
        both = both.astype(BF16).astype(F32)
        qrow[0, cc : cc + 1, :] = both[0:1]
        qrow[1, cc : cc + 1, :] = both[1:2]

    k_cp.wait()
    v_cp.wait()
    column = lax.broadcasted_iota(jnp.int32, (16, WIN), 1)
    for r in range(2):
        x = qrow[r]
        turned = x * cs_v[2 * r : 2 * r + 1, :] + pltpu.roll(x, 64, 1) * cs_v[2 * r + 1 : 2 * r + 2, :]
        query = turned.astype(BF16)
        rounded = query.astype(F32)
        new_key = rounded[12:13]
        new_value = x[13:14]
        slot_r = slots[row0 + r]
        pos_r = pos[row0 + r]
        hit = column == slot_r
        fresh = jnp.sum(rounded * new_key, axis=1, keepdims=True) * SCALE
        scores = lax.dot_general(query, k_v[r], NT, preferred_element_type=F32) * SCALE
        scores = jnp.where(hit, fresh, scores)
        usable = ((slot_r - column) & (WIN - 1)) <= pos_r
        scores = jnp.where(usable, scores, MASKED)
        highest = jnp.max(scores, axis=1, keepdims=True)
        weights = jnp.exp(scores - highest)
        denom = jnp.sum(weights, axis=1, keepdims=True)
        stale = jnp.where(hit, 0.0, weights).astype(BF16)
        summed = jnp.dot(stale, v_v[r], preferred_element_type=F32)
        own = jnp.exp(fresh - highest).astype(BF16).astype(F32)
        attended = ((summed + own * new_value) / denom).astype(BF16).astype(F32)
        for h in range(12):
            att_v[h, r : r + 1, :] = attended[h : h + 1]

    here = s * 16 + d16

    def spread_heads(n, carry):
        b, i = n // 16, n % 16
        u = i // 2

        @pl.when(jnp.logical_not((b == s) & (i == d16)))
        def _():
            pltpu.make_async_remote_copy(
                src_ref=att_v.at[pl.ds(3 * u // 2, 2)],
                dst_ref=recv2.at[here],
                send_sem=s2,
                recv_sem=r2,
                device_id=(b, 8 * z + u, i % 2),
                device_id_type=MESH,
            ).start()

        return carry

    lax.fori_loop(0, 32, spread_heads, 0)
    recv2[here] = att_v[pl.ds(3 * chip // 2, 2)]

    gu.wait()
    both = gu_send[...] + gu_recv[...]
    lane136 = lax.broadcasted_iota(jnp.int32, (FFB, 128), 1)
    active = both / (1.0 + jnp.exp(-both)) * pltpu.roll(both, 64, 1)
    act_v[c] = jnp.where(lane136 < 64, active, 0.0).astype(BF16)
    act_cp = pltpu.make_async_remote_copy(
        src_ref=act_v.at[c],
        dst_ref=act_v.at[c],
        send_sem=s4,
        recv_sem=r4,
        device_id=sibling,
        device_id_type=MESH,
    )
    act_cp.start()
    wd_cp.wait()
    pre_down.wait()
    act_cp.wait()
    for n in range(6):
        cols = slice(512 * n, 512 * n + 512)
        acc_v[:, cols] = lax.dot_general(
            act_v[0, :, 0:64], wd_v[0, :, cols], TN, preferred_element_type=F32
        ) + lax.dot_general(
            act_v[1, :, 0:64], wd_v[1, :, cols], TN, preferred_element_type=F32
        )
    wo_cp.wait()
    pre_out.wait()

    most = recv2.at[pl.ds(0, 31)]
    wait_recv(most, most, s2, r2)
    for n in range(32):
        lhs_v[2 * n : 2 * n + 2, 0:128] = recv2[n, 0]
        lhs_v[2 * n : 2 * n + 2, 128:256] = recv2[n, 1]
    lhs = lhs_v[...].astype(BF16)
    for n in range(6):
        low = slice(256 * n, 256 * n + 256)
        high = slice(1536 + 256 * n, 1536 + 256 * n + 256)
        pa = jnp.dot(lhs, wo_v[:, low], preferred_element_type=F32) + acc_v[:, low]
        pb = jnp.dot(lhs, wo_v[:, high], preferred_element_type=F32) + acc_v[:, high]
        turned = jnp.concatenate([pa, pb], axis=0).T.astype(BF16)
        for w in range(16):
            at = 256 * n + 16 * w
            zl, rest = divmod(at, 768)
            dd, e = divmod(rest, 48)
            p1send[zl, dd, e : e + 16, :] = turned[16 * w : 16 * w + 16]

    def scatter(n, carry):
        @pl.when(n != d16)
        def _():
            pltpu.make_async_remote_copy(
                src_ref=p1send.at[:, n],
                dst_ref=recvp1.at[d16],
                send_sem=sp1,
                recv_sem=rp1,
                device_id=(s, 8 * z + n // 2, n % 2),
                device_id_type=MESH,
            ).start()

        return carry

    lax.fori_loop(0, 16, scatter, 0)
    recvp1[d16] = p1send[:, d16]
    most1 = recvp1.at[pl.ds(0, 15)]
    wait_recv(most1, most1, sp1, rp1)
    lane24 = lax.broadcasted_iota(jnp.int32, (24, 128), 1) < 64
    for cs in range(2):
        for zl in range(2):
            part = recvp1[cs, zl].astype(F32)
            for p in range(1, 8):
                part = part + recvp1[2 * p + cs, zl].astype(F32)
            a, b = part[0:24], part[24:48]
            p2send[4 * cs + zl] = jnp.where(lane24, a, pltpu.roll(b, 64, 1)).astype(BF16)
            p2send[4 * cs + 2 + zl] = jnp.where(lane24, pltpu.roll(a, 64, 1), b).astype(BF16)

    def along(n, carry):
        @pl.when(n != z)
        def _():
            pltpu.make_async_remote_copy(
                src_ref=p2send.at[n],
                dst_ref=recvp2.at[z],
                send_sem=sp2,
                recv_sem=rp2,
                device_id=(s, 8 * n + chip, c),
                device_id_type=MESH,
            ).start()

        return carry

    lax.fori_loop(0, 8, along, 0)
    recvp2[z] = p2send[z]
    most2 = recvp2.at[pl.ds(0, 7)]
    wait_recv(most2, most2, sp2, rp2)
    last = recvp2[0].astype(F32)
    for n in range(1, 8):
        last = last + recvp2[n].astype(F32)
    result = jnp.concatenate([last, pltpu.roll(last, 64, 1)], axis=0)[:, 0:64]
    out[...] = (result + res_v[pl.ds(res_off, 48), :]).astype(BF16)

    edge = (t == 0) | (t == 7)
    for count, when in (
        (64, jnp.logical_not(edge) & jnp.logical_not(mine)),
        (63, jnp.logical_not(edge) & mine),
        (32, edge & jnp.logical_not(mine)),
        (31, edge & mine),
    ):

        @pl.when(when)
        def _():
            part = send1.at[pl.ds(0, count)]
            wait_send(part, part, s1, r1)

    wait_send(most, most, s2, r2)
    wait_send(most1, most1, sp1, rp1)
    wait_send(most2, most2, sp2, rp2)


def body(
    hidden, gain, qkv, out_w, gate, up, down, keys, values, positions, write_slots
):
    half = THETA ** (-2.0 * np.arange(64) / HD)
    freq = jnp.asarray(np.concatenate([half, half])[None, :].astype(np.float32))
    hbm = pl.BlockSpec(memory_space=pl.ANY)
    vmem = pl.BlockSpec(memory_space=pltpu.VMEM)
    smem = pl.BlockSpec(memory_space=pltpu.SMEM)
    dma = pltpu.SemaphoreType.DMA
    V = pltpu.VMEM
    result = pl.pallas_call(
        kernel,
        out_shape=jax.ShapeDtypeStruct((48, 64), BF16),
        in_specs=[hbm] * 9 + [smem, smem, vmem],
        out_specs=vmem,
        scratch_shapes=[
            V((64, D), BF16),
            V((96, 128), F32),
            V((128, HALF), BF16),
            V((256, NCOL), BF16),
            V((FFB, HALF), BF16),
            V((FFB, HALF), BF16),
            V((2, FFB, NCOL), BF16),
            V((2, WIN, HD), BF16),
            V((2, WIN, HD), BF16),
            V((64, HALF), BF16),
            V((64, 2, 128), F32),
            V((56, 2, 128), F32),
            V((2, 16, 128), F32),
            V((8, 128), F32),
            V((12, 2, 128), F32),
            V((32, 2, 2, 128), F32),
            V((64, 256), F32),
            V((FFB, 128), F32),
            V((FFB, 128), F32),
            V((2, FFB, 128), BF16),
            V((64, NCOL), F32),
            V((2, 16, 48, 128), BF16),
            V((16, 2, 48, 128), BF16),
            V((8, 24, 128), BF16),
            V((8, 24, 128), BF16),
            V((256, 64), F32),
            dma((9,)),
            dma, dma,
            dma((2,)), dma((2,)),
            dma, dma, dma, dma, dma, dma, dma, dma, dma, dma,
        ],
        compiler_params=pltpu.CompilerParams(
            collective_id=0, has_side_effects=True, vmem_limit_bytes=60 * 1024 * 1024
        ),
        name="layer",
    )(
        hidden,
        gain.reshape(96, 128),
        qkv.T,
        out_w,
        gate.T,
        up.T,
        down,
        keys,
        values,
        positions,
        write_slots,
        freq,
    )
    return result.T


def solution(mesh):
    side, grp, rep = mesh.axis_names
    inner = (grp, rep)
    every = (side, grp, rep)
    placed = (
        P(),
        P(),
        P(side, inner),
        P(inner, side),
        P(side, inner),
        P(side, inner),
        P(inner, side),
        P(every, None, None),
        P(every, None, None),
        P(),
        P(),
    )
    return jax.shard_map(
        body, mesh=mesh, in_specs=placed, out_specs=P(None, every), check_vma=False
    )
```

```python
import math

import jax
import jax.numpy as jnp
import numpy as np
from jax import lax
from jax.experimental import pallas as pl
from jax.experimental.pallas import tpu as pltpu
from jax.sharding import PartitionSpec as P

MESH = pl.DeviceIdType.MESH
D = 12288
HALF = 6144
EPSILON = 1e-05
THETA = 50000.0
MASKED = -1e30
WIN = 4096
HD = 128
COLS = 112
FFB = 136
OB = 96
NCOL = 3072
SCALE = 1.0 / math.sqrt(HD)
F32 = jnp.float32
BF16 = jnp.bfloat16


def div(a, b):
    return lax.div(a, jnp.int32(b))


def rem(a, b):
    return lax.rem(a, jnp.int32(b))


NT = (((1,), (1,)), ((), ()))
TN = (((0,), (0,)), ((), ()))


def kernel(
    hidden, gain, qkv, out_w, gate, up, down, keys, values, pos_h, slots_h, freq_h, out,
    hid_v, gain_v, qkv_v, wo_v, gate_v, up_v, wd_v, k_v, v_v, normed_v,
    send1, recv1, qrow, cs_v, att_v, recv2, lhs_v, gu_send, gu_recv, act_v, acc_v,
    p1send, recvp1, p2send, recvp2, res_v, pos, slots, freq,
    load_sem, s1, r1, spre, rpre, s2, r2, s3, r3, s4, r4, sp1, rp1, sp2, rp2,
):
    s = lax.axis_index("side")
    g = lax.axis_index("grp")
    c = lax.axis_index("rep")
    z = div(g, 8)
    chip = rem(g, 8)
    j = 2 * g + c
    d16 = 2 * chip + c
    row_off = 64 * (rem(chip, 2))

    def load(src, dst, n):
        cp = pltpu.make_async_copy(src, dst, load_sem.at[n])
        cp.start()
        return cp

    quarter = D // 4
    hid_cp = [
        load(
            hidden.at[:, pl.ds(quarter * n, quarter)],
            hid_v.at[:, pl.ds(quarter * n, quarter)],
            n,
        )
        for n in range(4)
    ]
    gain_cp = load(gain, gain_v, 4)
    qkv_cp = load(qkv, qkv_v.at[pl.ds(0, COLS)], 5)

    barrier = pltpu.get_barrier_semaphore()

    def greet(side, grp, rep):
        pl.semaphore_signal(
            barrier, inc=1, device_id=(side, grp, rep), device_id_type=MESH
        )

    source = 8 * div(z, 7) + rem(z, 7)
    left = rem(z, 7)
    for cc in range(14):
        for near in (source, source + 1):
            greet(1 - s, div(near, 2), rem(near, 2))

            @pl.when(near != j)
            def _():
                greet(s, div(near, 2), rem(near, 2))

        left = left + 1
        wrap = left == 7
        source = source + jnp.where(wrap, 10, 9)
        left = jnp.where(wrap, 0, left)
    for o in range(16):
        i = rem(d16 + o, 16)
        greet(1 - s, 8 * z + div(i, 2), rem(i, 2))
        if o > 0:
            greet(s, 8 * z + div(i, 2), rem(i, 2))
    for o in range(1, 8):
        greet(s, 8 * rem(z + o, 8) + chip, c)

    gate_cp = load(gate, gate_v, 6)
    up_cp = load(up, up_v, 7)
    k_cp = load(keys, k_v, 8)
    v_cp = load(values, v_v, 9)
    own_cols = pl.ds(pl.multiple_of(NCOL * c, NCOL), NCOL)
    wo_cp = load(
        out_w.at[:, own_cols], wo_v.at[pl.ds(pl.multiple_of(row_off + OB * c, 32), OB)], 10
    )
    wd_cp = load(down.at[:, own_cols], wd_v.at[c], 11)
    pos_cp = load(pos_h, pos, 12)
    slots_cp = load(slots_h, slots, 13)
    freq_cp = load(freq_h, freq, 14)

    qkv_v[pl.ds(COLS, 16), :] = jnp.zeros((16, HALF), BF16)
    wo_v[pl.ds(pl.multiple_of(192 - 192 * (rem(chip, 2)), 64), 64), :] = jnp.zeros((64, NCOL), BF16)


    def chunk(i):
        return hid_v[:, pl.ds(pl.multiple_of(i * 128, 128), 128)].astype(F32)

    total = jnp.zeros((64, 128), F32)
    for n in range(4):
        hid_cp[n].wait()
        total = lax.fori_loop(24 * n, 24 * n + 24, lambda i, a: a + chunk(i), total, unroll=8)
    mean = jnp.sum(total, axis=1, keepdims=True) * (1.0 / D)

    def square(i, a):
        d = chunk(i) - mean
        return a + d * d

    spread = lax.fori_loop(0, 96, square, jnp.zeros((64, 128), F32), unroll=8)
    var = jnp.sum(spread, axis=1, keepdims=True) * (1.0 / D)
    rstd = lax.rsqrt(var + EPSILON)
    gain_cp.wait()

    def norm(i, carry):
        n = s * 48 + i
        v = (chunk(n) - mean) * rstd * gain_v[pl.ds(n, 1), :]
        normed_v[:, pl.ds(pl.multiple_of(i * 128, 128), 128)] = v.astype(BF16)
        return carry

    lax.fori_loop(0, 48, norm, 0, unroll=4)

    qkv_cp.wait()
    term = lax.dot_general(normed_v[...], qkv_v[...], NT, preferred_element_type=F32)
    m, t = div(j, 8), rem(j, 8)
    rolled = pltpu.roll(term, (128 - 16 * t) % 128, 1)
    lane = lax.broadcasted_iota(jnp.int32, (64, 128), 1)
    first = jnp.where(lane < COLS - 16 * t, rolled, 0.0)
    second = jnp.where(lane >= 128 - 16 * t, rolled, 0.0)
    for n in range(32):
        send1[n] = first[2 * n : 2 * n + 2]
        send1[32 + n] = second[2 * n : 2 * n + 2]

    mine = ((t <= 6) & (rem(7 * m + t, 8) == z)) | ((t >= 1) & (rem(7 * m + t + 7, 8) == z))
    edge = (t == 0) | (t == 7)
    pl.semaphore_wait(barrier, jnp.where(edge, 70, 102) - jnp.where(mine, 1, 0))

    valid = (t <= 6, t >= 1)
    for piece in range(2):
        q = jnp.maximum(7 * m + t - piece, 0)
        k, cc = rem(q, 8), div(q, 8)
        slot = jnp.minimum(cc, 13) * 4 + piece * 2 + s

        @pl.when(valid[piece])
        def _():
            def push(b, i):
                pltpu.make_async_remote_copy(
                    src_ref=send1.at[32 * piece + 16 * b + i],
                    dst_ref=recv1.at[slot],
                    send_sem=s1,
                    recv_sem=r1,
                    device_id=(b, 8 * k + div(i, 2), rem(i, 2)),
                    device_id_type=MESH,
                ).start()

            for o in range(16):
                i = rem(d16 + o, 16)
                push(1 - s, i)
                if o > 0:
                    push(s, i)

            @pl.when(k != z)
            def _():
                push(s, d16)

            @pl.when(k == z)
            def _():
                recv1[slot] = send1[32 * piece + s * 16 + d16]

    other_cols = pl.ds(pl.multiple_of(NCOL * (1 - c), NCOL), NCOL)
    sibling = (s, g, 1 - c)
    pre_out = pltpu.make_async_remote_copy(
        src_ref=out_w.at[:, other_cols],
        dst_ref=wo_v.at[pl.ds(pl.multiple_of(row_off + OB * c, 32), OB)],
        send_sem=spre.at[0],
        recv_sem=rpre.at[0],
        device_id=sibling,
        device_id_type=MESH,
    )
    pre_out.start()
    pre_down = pltpu.make_async_remote_copy(
        src_ref=down.at[:, other_cols],
        dst_ref=wd_v.at[c],
        send_sem=spre.at[1],
        recv_sem=rpre.at[1],
        device_id=sibling,
        device_id_type=MESH,
    )
    pre_down.start()

    gate_cp.wait()
    gu_send[:, 0:64] = lax.dot_general(
        gate_v[...], normed_v[...], NT, preferred_element_type=F32
    )
    up_cp.wait()
    gu_send[:, 64:128] = lax.dot_general(
        up_v[...], normed_v[...], NT, preferred_element_type=F32
    )
    gu = pltpu.make_async_remote_copy(
        src_ref=gu_send,
        dst_ref=gu_recv,
        send_sem=s3,
        recv_sem=r3,
        device_id=(1 - s, g, c),
        device_id_type=MESH,
    )
    gu.start()

    col0 = 48 * (128 * s + j)
    tile = jnp.minimum(div(col0, 128), 94)
    res_v[...] = hid_v[:, pl.ds(pl.multiple_of(tile * 128, 128), 256)].astype(F32).T
    res_off = pl.multiple_of(col0 - tile * 128, 16)

    lane1 = lax.broadcasted_iota(jnp.int32, (1, 128), 1)
    row0 = 32 * s + 2 * d16
    pos_cp.wait()
    slots_cp.wait()
    freq_cp.wait()
    for r in range(2):
        angle = pos[row0 + r].astype(F32) * freq[...]
        sine = jnp.sin(angle)
        cs_v[2 * r : 2 * r + 1, :] = jnp.cos(angle)
        cs_v[2 * r + 1 : 2 * r + 2, :] = jnp.where(lane1 < 64, -sine, sine)
    qrow[...] = jnp.zeros((2, 16, 128), F32)

    def wait_recv(src, dst, send, recv):
        pltpu.make_async_remote_copy(
            src_ref=src, dst_ref=dst, send_sem=send, recv_sem=recv,
            device_id=sibling, device_id_type=MESH,
        ).wait_recv()

    def wait_send(src, dst, send, recv):
        pltpu.make_async_remote_copy(
            src_ref=src, dst_ref=dst, send_sem=send, recv_sem=recv,
            device_id=sibling, device_id_type=MESH,
        ).wait_send()

    @pl.when(mine)
    def _():
        part = recv1.at[pl.ds(0, 55)]
        wait_recv(part, part, s1, r1)

    @pl.when(jnp.logical_not(mine))
    def _():
        wait_recv(recv1, recv1, s1, r1)

    for cc in range(14):
        both = (recv1[4 * cc] + recv1[4 * cc + 1]) + (recv1[4 * cc + 2] + recv1[4 * cc + 3])
        both = both.astype(BF16).astype(F32)
        qrow[0, cc : cc + 1, :] = both[0:1]
        qrow[1, cc : cc + 1, :] = both[1:2]

    k_cp.wait()
    v_cp.wait()
    column = lax.broadcasted_iota(jnp.int32, (16, WIN), 1)
    for r in range(2):
        x = qrow[r]
        turned = x * cs_v[2 * r : 2 * r + 1, :] + pltpu.roll(x, 64, 1) * cs_v[2 * r + 1 : 2 * r + 2, :]
        query = turned.astype(BF16)
        rounded = query.astype(F32)
        new_key = rounded[12:13]
        new_value = x[13:14]
        slot_r = slots[row0 + r]
        pos_r = pos[row0 + r]
        hit = column == slot_r
        fresh = jnp.sum(rounded * new_key, axis=1, keepdims=True) * SCALE
        scores = lax.dot_general(query, k_v[r], NT, preferred_element_type=F32) * SCALE
        scores = jnp.where(hit, fresh, scores)
        usable = ((slot_r - column) & (WIN - 1)) <= pos_r
        scores = jnp.where(usable, scores, MASKED)
        highest = jnp.max(scores, axis=1, keepdims=True)
        weights = jnp.exp(scores - highest)
        denom = jnp.sum(weights, axis=1, keepdims=True)
        stale = jnp.where(hit, 0.0, weights).astype(BF16)
        summed = jnp.dot(stale, v_v[r], preferred_element_type=F32)
        own = jnp.exp(fresh - highest).astype(BF16).astype(F32)
        attended = ((summed + own * new_value) / denom).astype(BF16).astype(F32)
        for h in range(12):
            att_v[h, r : r + 1, :] = attended[h : h + 1]

    here = s * 16 + d16

    def spread_heads(b, i):
        u = div(i, 2)
        pltpu.make_async_remote_copy(
            src_ref=att_v.at[pl.ds(div(3 * u, 2), 2)],
            dst_ref=recv2.at[here],
            send_sem=s2,
            recv_sem=r2,
            device_id=(b, 8 * z + u, rem(i, 2)),
            device_id_type=MESH,
        ).start()

    for o in range(16):
        i = rem(d16 + o, 16)
        spread_heads(1 - s, i)
        if o > 0:
            spread_heads(s, i)
    recv2[here] = att_v[pl.ds(div(3 * chip, 2), 2)]

    gu.wait()
    both = gu_send[...] + gu_recv[...]
    lane136 = lax.broadcasted_iota(jnp.int32, (FFB, 128), 1)
    active = both / (1.0 + jnp.exp(-both)) * pltpu.roll(both, 64, 1)
    act_v[c] = jnp.where(lane136 < 64, active, 0.0).astype(BF16)
    act_cp = pltpu.make_async_remote_copy(
        src_ref=act_v.at[c],
        dst_ref=act_v.at[c],
        send_sem=s4,
        recv_sem=r4,
        device_id=sibling,
        device_id_type=MESH,
    )
    act_cp.start()
    wd_cp.wait()
    pre_down.wait()
    act_cp.wait()
    for n in range(6):
        cols = slice(512 * n, 512 * n + 512)
        acc_v[:, cols] = lax.dot_general(
            act_v[0, :, 0:64], wd_v[0, :, cols], TN, preferred_element_type=F32
        ) + lax.dot_general(
            act_v[1, :, 0:64], wd_v[1, :, cols], TN, preferred_element_type=F32
        )
    wo_cp.wait()
    pre_out.wait()

    most = recv2.at[pl.ds(0, 31)]
    wait_recv(most, most, s2, r2)
    for n in range(32):
        lhs_v[2 * n : 2 * n + 2, 0:128] = recv2[n, 0]
        lhs_v[2 * n : 2 * n + 2, 128:256] = recv2[n, 1]
    lhs = lhs_v[...].astype(BF16)
    for n in range(6):
        low = slice(256 * n, 256 * n + 256)
        high = slice(1536 + 256 * n, 1536 + 256 * n + 256)
        pa = jnp.dot(lhs, wo_v[:, low], preferred_element_type=F32) + acc_v[:, low]
        pb = jnp.dot(lhs, wo_v[:, high], preferred_element_type=F32) + acc_v[:, high]
        turned = jnp.concatenate([pa, pb], axis=0).T.astype(BF16)
        for w in range(16):
            at = 256 * n + 16 * w
            zl, rest = divmod(at, 768)
            dd, e = divmod(rest, 48)
            p1send[zl, dd, e : e + 16, :] = turned[16 * w : 16 * w + 16]

    for o in range(1, 16):
        n = rem(d16 + o, 16)
        pltpu.make_async_remote_copy(
            src_ref=p1send.at[:, n],
            dst_ref=recvp1.at[d16],
            send_sem=sp1,
            recv_sem=rp1,
            device_id=(s, 8 * z + div(n, 2), rem(n, 2)),
            device_id_type=MESH,
        ).start()
    recvp1[d16] = p1send[:, d16]
    most1 = recvp1.at[pl.ds(0, 15)]
    wait_recv(most1, most1, sp1, rp1)
    lane24 = lax.broadcasted_iota(jnp.int32, (24, 128), 1) < 64
    for cs in range(2):
        for zl in range(2):
            part = recvp1[cs, zl].astype(F32)
            for p in range(1, 8):
                part = part + recvp1[2 * p + cs, zl].astype(F32)
            a, b = part[0:24], part[24:48]
            p2send[4 * cs + zl] = jnp.where(lane24, a, pltpu.roll(b, 64, 1)).astype(BF16)
            p2send[4 * cs + 2 + zl] = jnp.where(lane24, pltpu.roll(a, 64, 1), b).astype(BF16)

    for o in range(1, 8):
        n = rem(z + o, 8)
        pltpu.make_async_remote_copy(
            src_ref=p2send.at[n],
            dst_ref=recvp2.at[z],
            send_sem=sp2,
            recv_sem=rp2,
            device_id=(s, 8 * n + chip, c),
            device_id_type=MESH,
        ).start()
    recvp2[z] = p2send[z]
    most2 = recvp2.at[pl.ds(0, 7)]
    wait_recv(most2, most2, sp2, rp2)
    last = recvp2[0].astype(F32)
    for n in range(1, 8):
        last = last + recvp2[n].astype(F32)
    result = jnp.concatenate([last, pltpu.roll(last, 64, 1)], axis=0)[:, 0:64]
    out[...] = (result + res_v[pl.ds(res_off, 48), :]).astype(BF16)

    for count, when in (
        (64, jnp.logical_not(edge) & jnp.logical_not(mine)),
        (63, jnp.logical_not(edge) & mine),
        (32, edge & jnp.logical_not(mine)),
        (31, edge & mine),
    ):

        @pl.when(when)
        def _():
            part = send1.at[pl.ds(0, count)]
            wait_send(part, part, s1, r1)

    wait_send(most, most, s2, r2)
    wait_send(most1, most1, sp1, rp1)
    wait_send(most2, most2, sp2, rp2)


def body(
    hidden, gain, qkv, out_w, gate, up, down, keys, values, positions, write_slots
):
    half = THETA ** (-2.0 * np.arange(64) / HD)
    freq = jnp.asarray(np.concatenate([half, half])[None, :].astype(np.float32))
    hbm = pl.BlockSpec(memory_space=pl.ANY)
    vmem = pl.BlockSpec(memory_space=pltpu.VMEM)
    dma = pltpu.SemaphoreType.DMA
    V = pltpu.VMEM
    result = pl.pallas_call(
        kernel,
        out_shape=jax.ShapeDtypeStruct((48, 64), BF16),
        in_specs=[hbm] * 12,
        out_specs=vmem,
        scratch_shapes=[
            V((64, D), BF16),
            V((96, 128), F32),
            V((128, HALF), BF16),
            V((256, NCOL), BF16),
            V((FFB, HALF), BF16),
            V((FFB, HALF), BF16),
            V((2, FFB, NCOL), BF16),
            V((2, WIN, HD), BF16),
            V((2, WIN, HD), BF16),
            V((64, HALF), BF16),
            V((64, 2, 128), F32),
            V((56, 2, 128), F32),
            V((2, 16, 128), F32),
            V((8, 128), F32),
            V((12, 2, 128), F32),
            V((32, 2, 2, 128), F32),
            V((64, 256), F32),
            V((FFB, 128), F32),
            V((FFB, 128), F32),
            V((2, FFB, 128), BF16),
            V((64, NCOL), F32),
            V((2, 16, 48, 128), BF16),
            V((16, 2, 48, 128), BF16),
            V((8, 24, 128), BF16),
            V((8, 24, 128), BF16),
            V((256, 64), F32),
            pltpu.SMEM((64,), jnp.int32),
            pltpu.SMEM((64,), jnp.int32),
            V((1, 128), F32),
            dma((15,)),
            dma, dma,
            dma((2,)), dma((2,)),
            dma, dma, dma, dma, dma, dma, dma, dma, dma, dma,
        ],
        compiler_params=pltpu.CompilerParams(
            collective_id=0, has_side_effects=True, vmem_limit_bytes=60 * 1024 * 1024
        ),
        name="layer",
    )(
        hidden,
        gain.reshape(96, 128),
        qkv.T,
        out_w,
        gate.T,
        up.T,
        down,
        keys,
        values,
        positions,
        write_slots,
        freq,
    )
    return result.T


def solution(mesh):
    side, grp, rep = mesh.axis_names
    inner = (grp, rep)
    every = (side, grp, rep)
    placed = (
        P(),
        P(),
        P(side, inner),
        P(inner, side),
        P(side, inner),
        P(side, inner),
        P(inner, side),
        P(every, None, None),
        P(every, None, None),
        P(),
        P(),
    )
    return jax.shard_map(
        body, mesh=mesh, in_specs=placed, out_specs=P(None, every), check_vma=False
    )
```

```python
import math

import jax
import jax.numpy as jnp
import numpy as np
from jax import lax
from jax.experimental import pallas as pl
from jax.experimental.pallas import tpu as pltpu
from jax.sharding import PartitionSpec as P

MESH = pl.DeviceIdType.MESH
D = 12288
HALF = 6144
EPSILON = 1e-05
THETA = 50000.0
MASKED = -1e30
WIN = 4096
HD = 128
COLS = 112
FFB = 136
OB = 96
NCOL = 3072
SCALE = 1.0 / math.sqrt(HD)
F32 = jnp.float32
BF16 = jnp.bfloat16


def div(a, b):
    return lax.div(a, jnp.int32(b))


def rem(a, b):
    return lax.rem(a, jnp.int32(b))


NT = (((1,), (1,)), ((), ()))
TN = (((0,), (0,)), ((), ()))


def kernel(
    hidden, gain, qkv, out_w, gate, up, down, keys, values, pos_h, slots_h, freq_h, out,
    hid_v, gain_v, qkv_v, wo_v, gate_v, up_v, wd_v, k_v, v_v, normed_v,
    send1, recv1, qrow, cs_v, att_v, recv2, lhs_v, gu_send, gu_recv, act_v, acc_v,
    p1send, recvp1, p2send, recvp2, res_v, pos, slots, freq,
    load_sem, s1, r1, spre, rpre, s2, r2, s3, r3, s4, r4, sp1, rp1, sp2, rp2,
):
    s = lax.axis_index("side")
    g = lax.axis_index("grp")
    c = lax.axis_index("rep")
    z = div(g, 8)
    chip = rem(g, 8)
    j = 2 * g + c
    d16 = 2 * chip + c
    row_off = 64 * (rem(chip, 2))

    def load(src, dst, n):
        cp = pltpu.make_async_copy(src, dst, load_sem.at[n])
        cp.start()
        return cp

    quarter = D // 4
    hid_cp = [
        load(
            hidden.at[:, pl.ds(quarter * n, quarter)],
            hid_v.at[:, pl.ds(quarter * n, quarter)],
            n,
        )
        for n in range(4)
    ]
    gain_cp = load(gain, gain_v, 4)
    qkv_cp = load(qkv, qkv_v.at[pl.ds(0, COLS)], 5)

    barrier = pltpu.get_barrier_semaphore()

    def greet(side, grp, rep):
        pl.semaphore_signal(
            barrier, inc=1, device_id=(side, grp, rep), device_id_type=MESH
        )

    source = 8 * div(z, 7) + rem(z, 7)
    left = rem(z, 7)
    for cc in range(14):
        for near in (source, source + 1):
            greet(1 - s, div(near, 2), rem(near, 2))

            @pl.when(near != j)
            def _():
                greet(s, div(near, 2), rem(near, 2))

        left = left + 1
        wrap = left == 7
        source = source + jnp.where(wrap, 10, 9)
        left = jnp.where(wrap, 0, left)
    for o in range(16):
        i = rem(d16 + o, 16)
        greet(1 - s, 8 * z + div(i, 2), rem(i, 2))
        if o > 0:
            greet(s, 8 * z + div(i, 2), rem(i, 2))
    for o in range(1, 8):
        greet(s, 8 * rem(z + o, 8) + chip, c)

    gate_cp = load(gate, gate_v, 6)
    up_cp = load(up, up_v, 7)
    k_cp = load(keys, k_v, 8)
    v_cp = load(values, v_v, 9)
    own_cols = pl.ds(pl.multiple_of(NCOL * c, NCOL), NCOL)
    wo_cp = load(
        out_w.at[:, own_cols], wo_v.at[pl.ds(pl.multiple_of(row_off + OB * c, 32), OB)], 10
    )
    wd_cp = load(down.at[:, own_cols], wd_v.at[c], 11)
    pos_cp = load(pos_h, pos, 12)
    slots_cp = load(slots_h, slots, 13)
    freq_cp = load(freq_h, freq, 14)

    qkv_v[pl.ds(COLS, 16), :] = jnp.zeros((16, HALF), BF16)
    wo_v[pl.ds(pl.multiple_of(192 - 192 * (rem(chip, 2)), 64), 64), :] = jnp.zeros((64, NCOL), BF16)


    def chunk(i):
        return hid_v[:, pl.ds(pl.multiple_of(i * 128, 128), 128)].astype(F32)

    hid_cp[0].wait()
    pivot = jnp.sum(chunk(0), axis=1, keepdims=True) * (1.0 / 128)

    def moments(i, carry):
        one, two = carry
        d = chunk(i) - pivot
        return one + d, two + d * d

    carry = (jnp.zeros((64, 128), F32), jnp.zeros((64, 128), F32))
    for n in range(4):
        if n > 0:
            hid_cp[n].wait()
        carry = lax.fori_loop(24 * n, 24 * n + 24, moments, carry, unroll=8)
    shift = jnp.sum(carry[0], axis=1, keepdims=True) * (1.0 / D)
    mean = pivot + shift
    var = jnp.sum(carry[1], axis=1, keepdims=True) * (1.0 / D) - shift * shift
    rstd = lax.rsqrt(jnp.maximum(var, 0.0) + EPSILON)
    gain_cp.wait()
    qkv_cp.wait()

    term = jnp.zeros((64, 128), F32)
    for n in range(12):
        for w in range(4):
            at = 4 * n + w
            v = (chunk(s * 48 + at) - mean) * rstd * gain_v[pl.ds(s * 48 + at, 1), :]
            normed_v[:, 128 * at : 128 * at + 128] = v.astype(BF16)
        cols = slice(512 * n, 512 * n + 512)
        term = term + lax.dot_general(
            normed_v[:, cols], qkv_v[:, cols], NT, preferred_element_type=F32
        )
    m, t = div(j, 8), rem(j, 8)
    rolled = pltpu.roll(term, (128 - 16 * t) % 128, 1)
    lane = lax.broadcasted_iota(jnp.int32, (64, 128), 1)
    first = jnp.where(lane < COLS - 16 * t, rolled, 0.0)
    second = jnp.where(lane >= 128 - 16 * t, rolled, 0.0)
    for n in range(32):
        send1[n] = first[2 * n : 2 * n + 2]
        send1[32 + n] = second[2 * n : 2 * n + 2]

    mine = ((t <= 6) & (rem(7 * m + t, 8) == z)) | ((t >= 1) & (rem(7 * m + t + 7, 8) == z))
    edge = (t == 0) | (t == 7)
    pl.semaphore_wait(barrier, jnp.where(edge, 70, 102) - jnp.where(mine, 1, 0))

    valid = (t <= 6, t >= 1)
    for piece in range(2):
        q = jnp.maximum(7 * m + t - piece, 0)
        k, cc = rem(q, 8), div(q, 8)
        slot = jnp.minimum(cc, 13) * 4 + piece * 2 + s

        @pl.when(valid[piece])
        def _():
            def push(b, i):
                pltpu.make_async_remote_copy(
                    src_ref=send1.at[32 * piece + 16 * b + i],
                    dst_ref=recv1.at[slot],
                    send_sem=s1,
                    recv_sem=r1,
                    device_id=(b, 8 * k + div(i, 2), rem(i, 2)),
                    device_id_type=MESH,
                ).start()

            for o in range(16):
                i = rem(d16 + o, 16)
                push(1 - s, i)
                if o > 0:
                    push(s, i)

            @pl.when(k != z)
            def _():
                push(s, d16)

            @pl.when(k == z)
            def _():
                recv1[slot] = send1[32 * piece + s * 16 + d16]

    other_cols = pl.ds(pl.multiple_of(NCOL * (1 - c), NCOL), NCOL)
    sibling = (s, g, 1 - c)
    pre_out = pltpu.make_async_remote_copy(
        src_ref=out_w.at[:, other_cols],
        dst_ref=wo_v.at[pl.ds(pl.multiple_of(row_off + OB * c, 32), OB)],
        send_sem=spre.at[0],
        recv_sem=rpre.at[0],
        device_id=sibling,
        device_id_type=MESH,
    )
    pre_out.start()
    pre_down = pltpu.make_async_remote_copy(
        src_ref=down.at[:, other_cols],
        dst_ref=wd_v.at[c],
        send_sem=spre.at[1],
        recv_sem=rpre.at[1],
        device_id=sibling,
        device_id_type=MESH,
    )
    pre_down.start()

    gate_cp.wait()
    gu_send[:, 0:64] = lax.dot_general(
        gate_v[...], normed_v[...], NT, preferred_element_type=F32
    )
    up_cp.wait()
    gu_send[:, 64:128] = lax.dot_general(
        up_v[...], normed_v[...], NT, preferred_element_type=F32
    )
    gu = pltpu.make_async_remote_copy(
        src_ref=gu_send,
        dst_ref=gu_recv,
        send_sem=s3,
        recv_sem=r3,
        device_id=(1 - s, g, c),
        device_id_type=MESH,
    )
    gu.start()

    col0 = 48 * (128 * s + j)
    tile = jnp.minimum(div(col0, 128), 94)
    res_v[...] = hid_v[:, pl.ds(pl.multiple_of(tile * 128, 128), 256)].astype(F32).T
    res_off = pl.multiple_of(col0 - tile * 128, 16)

    lane1 = lax.broadcasted_iota(jnp.int32, (1, 128), 1)
    row0 = 32 * s + 2 * d16
    pos_cp.wait()
    slots_cp.wait()
    freq_cp.wait()
    for r in range(2):
        angle = pos[row0 + r].astype(F32) * freq[...]
        sine = jnp.sin(angle)
        cs_v[2 * r : 2 * r + 1, :] = jnp.cos(angle)
        cs_v[2 * r + 1 : 2 * r + 2, :] = jnp.where(lane1 < 64, -sine, sine)
    qrow[...] = jnp.zeros((2, 16, 128), F32)

    def wait_recv(src, dst, send, recv):
        pltpu.make_async_remote_copy(
            src_ref=src, dst_ref=dst, send_sem=send, recv_sem=recv,
            device_id=sibling, device_id_type=MESH,
        ).wait_recv()

    def wait_send(src, dst, send, recv):
        pltpu.make_async_remote_copy(
            src_ref=src, dst_ref=dst, send_sem=send, recv_sem=recv,
            device_id=sibling, device_id_type=MESH,
        ).wait_send()

    @pl.when(mine)
    def _():
        part = recv1.at[pl.ds(0, 55)]
        wait_recv(part, part, s1, r1)

    @pl.when(jnp.logical_not(mine))
    def _():
        wait_recv(recv1, recv1, s1, r1)

    for cc in range(14):
        both = (recv1[4 * cc] + recv1[4 * cc + 1]) + (recv1[4 * cc + 2] + recv1[4 * cc + 3])
        both = both.astype(BF16).astype(F32)
        qrow[0, cc : cc + 1, :] = both[0:1]
        qrow[1, cc : cc + 1, :] = both[1:2]

    k_cp.wait()
    v_cp.wait()
    column = lax.broadcasted_iota(jnp.int32, (16, WIN), 1)
    for r in range(2):
        x = qrow[r]
        turned = x * cs_v[2 * r : 2 * r + 1, :] + pltpu.roll(x, 64, 1) * cs_v[2 * r + 1 : 2 * r + 2, :]
        query = turned.astype(BF16)
        rounded = query.astype(F32)
        new_key = rounded[12:13]
        new_value = x[13:14]
        slot_r = slots[row0 + r]
        pos_r = pos[row0 + r]
        hit = column == slot_r
        fresh = jnp.sum(rounded * new_key, axis=1, keepdims=True) * SCALE
        scores = lax.dot_general(query, k_v[r], NT, preferred_element_type=F32) * SCALE
        scores = jnp.where(hit, fresh, scores)
        usable = ((slot_r - column) & (WIN - 1)) <= pos_r
        scores = jnp.where(usable, scores, MASKED)
        highest = jnp.max(scores, axis=1, keepdims=True)
        weights = jnp.exp(scores - highest)
        denom = jnp.sum(weights, axis=1, keepdims=True)
        stale = jnp.where(hit, 0.0, weights).astype(BF16)
        summed = jnp.dot(stale, v_v[r], preferred_element_type=F32)
        own = jnp.exp(fresh - highest).astype(BF16).astype(F32)
        attended = ((summed + own * new_value) / denom).astype(BF16).astype(F32)
        for h in range(12):
            att_v[h, r : r + 1, :] = attended[h : h + 1]

    here = s * 16 + d16

    def spread_heads(b, i):
        u = div(i, 2)
        pltpu.make_async_remote_copy(
            src_ref=att_v.at[pl.ds(div(3 * u, 2), 2)],
            dst_ref=recv2.at[here],
            send_sem=s2,
            recv_sem=r2,
            device_id=(b, 8 * z + u, rem(i, 2)),
            device_id_type=MESH,
        ).start()

    for o in range(16):
        i = rem(d16 + o, 16)
        spread_heads(1 - s, i)
        if o > 0:
            spread_heads(s, i)
    recv2[here] = att_v[pl.ds(div(3 * chip, 2), 2)]

    gu.wait()
    both = gu_send[...] + gu_recv[...]
    lane136 = lax.broadcasted_iota(jnp.int32, (FFB, 128), 1)
    active = both / (1.0 + jnp.exp(-both)) * pltpu.roll(both, 64, 1)
    act_v[c] = jnp.where(lane136 < 64, active, 0.0).astype(BF16)
    act_cp = pltpu.make_async_remote_copy(
        src_ref=act_v.at[c],
        dst_ref=act_v.at[c],
        send_sem=s4,
        recv_sem=r4,
        device_id=sibling,
        device_id_type=MESH,
    )
    act_cp.start()
    wd_cp.wait()
    pre_down.wait()
    act_cp.wait()
    for n in range(6):
        cols = slice(512 * n, 512 * n + 512)
        acc_v[:, cols] = lax.dot_general(
            act_v[0, :, 0:64], wd_v[0, :, cols], TN, preferred_element_type=F32
        ) + lax.dot_general(
            act_v[1, :, 0:64], wd_v[1, :, cols], TN, preferred_element_type=F32
        )
    wo_cp.wait()
    pre_out.wait()

    most = recv2.at[pl.ds(0, 31)]
    wait_recv(most, most, s2, r2)
    for n in range(32):
        lhs_v[2 * n : 2 * n + 2, 0:128] = recv2[n, 0]
        lhs_v[2 * n : 2 * n + 2, 128:256] = recv2[n, 1]
    lhs = lhs_v[...].astype(BF16)
    def scatter(zl):
        for o in range(1, 16):
            n = rem(d16 + o, 16)
            pltpu.make_async_remote_copy(
                src_ref=p1send.at[zl, n],
                dst_ref=recvp1.at[d16, zl],
                send_sem=sp1,
                recv_sem=rp1,
                device_id=(s, 8 * z + div(n, 2), rem(n, 2)),
                device_id_type=MESH,
            ).start()

    for n in range(6):
        low = slice(256 * n, 256 * n + 256)
        high = slice(1536 + 256 * n, 1536 + 256 * n + 256)
        pa = jnp.dot(lhs, wo_v[:, low], preferred_element_type=F32) + acc_v[:, low]
        pb = jnp.dot(lhs, wo_v[:, high], preferred_element_type=F32) + acc_v[:, high]
        turned = jnp.concatenate([pa, pb], axis=0).T.astype(BF16)
        for w in range(16):
            at = 256 * n + 16 * w
            zl, rest = divmod(at, 768)
            dd, e = divmod(rest, 48)
            p1send[zl, dd, e : e + 16, :] = turned[16 * w : 16 * w + 16]

    scatter(0)
    scatter(1)
    recvp1[d16] = p1send[:, d16]
    most1 = recvp1.at[pl.ds(0, 15)]
    wait_recv(most1, most1, sp1, rp1)
    lane24 = lax.broadcasted_iota(jnp.int32, (24, 128), 1) < 64
    for cs in range(2):
        for zl in range(2):
            part = recvp1[cs, zl].astype(F32)
            for p in range(1, 8):
                part = part + recvp1[2 * p + cs, zl].astype(F32)
            a, b = part[0:24], part[24:48]
            p2send[4 * cs + zl] = jnp.where(lane24, a, pltpu.roll(b, 64, 1)).astype(BF16)
            p2send[4 * cs + 2 + zl] = jnp.where(lane24, pltpu.roll(a, 64, 1), b).astype(BF16)

    for o in range(1, 8):
        n = rem(z + o, 8)
        pltpu.make_async_remote_copy(
            src_ref=p2send.at[n],
            dst_ref=recvp2.at[z],
            send_sem=sp2,
            recv_sem=rp2,
            device_id=(s, 8 * n + chip, c),
            device_id_type=MESH,
        ).start()
    recvp2[z] = p2send[z]
    most2 = recvp2.at[pl.ds(0, 7)]
    wait_recv(most2, most2, sp2, rp2)
    last = recvp2[0].astype(F32)
    for n in range(1, 8):
        last = last + recvp2[n].astype(F32)
    result = jnp.concatenate([last, pltpu.roll(last, 64, 1)], axis=0)[:, 0:64]
    out[...] = (result + res_v[pl.ds(res_off, 48), :]).astype(BF16)

    for count, when in (
        (64, jnp.logical_not(edge) & jnp.logical_not(mine)),
        (63, jnp.logical_not(edge) & mine),
        (32, edge & jnp.logical_not(mine)),
        (31, edge & mine),
    ):

        @pl.when(when)
        def _():
            part = send1.at[pl.ds(0, count)]
            wait_send(part, part, s1, r1)

    wait_send(most, most, s2, r2)
    wait_send(most1, most1, sp1, rp1)
    wait_send(most2, most2, sp2, rp2)


def body(
    hidden, gain, qkv, out_w, gate, up, down, keys, values, positions, write_slots
):
    half = THETA ** (-2.0 * np.arange(64) / HD)
    freq = jnp.asarray(np.concatenate([half, half])[None, :].astype(np.float32))
    hbm = pl.BlockSpec(memory_space=pl.ANY)
    vmem = pl.BlockSpec(memory_space=pltpu.VMEM)
    dma = pltpu.SemaphoreType.DMA
    V = pltpu.VMEM
    result = pl.pallas_call(
        kernel,
        out_shape=pltpu.VMEM((48, 64), BF16),
        in_specs=[hbm] * 12,
        out_specs=vmem,
        scratch_shapes=[
            V((64, D), BF16),
            V((96, 128), F32),
            V((128, HALF), BF16),
            V((256, NCOL), BF16),
            V((FFB, HALF), BF16),
            V((FFB, HALF), BF16),
            V((2, FFB, NCOL), BF16),
            V((2, WIN, HD), BF16),
            V((2, WIN, HD), BF16),
            V((64, HALF), BF16),
            V((64, 2, 128), F32),
            V((56, 2, 128), F32),
            V((2, 16, 128), F32),
            V((8, 128), F32),
            V((12, 2, 128), F32),
            V((32, 2, 2, 128), F32),
            V((64, 256), F32),
            V((FFB, 128), F32),
            V((FFB, 128), F32),
            V((2, FFB, 128), BF16),
            V((64, NCOL), F32),
            V((2, 16, 48, 128), BF16),
            V((16, 2, 48, 128), BF16),
            V((8, 24, 128), BF16),
            V((8, 24, 128), BF16),
            V((256, 64), F32),
            pltpu.SMEM((64,), jnp.int32),
            pltpu.SMEM((64,), jnp.int32),
            V((1, 128), F32),
            dma((15,)),
            dma, dma,
            dma((2,)), dma((2,)),
            dma, dma, dma, dma, dma, dma, dma, dma, dma, dma,
        ],
        compiler_params=pltpu.CompilerParams(
            collective_id=0, has_side_effects=True, vmem_limit_bytes=60 * 1024 * 1024
        ),
        name="layer",
    )(
        hidden,
        gain.reshape(96, 128),
        qkv.T,
        out_w,
        gate.T,
        up.T,
        down,
        keys,
        values,
        positions,
        write_slots,
        freq,
    )
    return result.T


def solution(mesh):
    side, grp, rep = mesh.axis_names
    inner = (grp, rep)
    every = (side, grp, rep)
    placed = (
        P(),
        P(),
        P(side, inner),
        P(inner, side),
        P(side, inner),
        P(side, inner),
        P(inner, side),
        P(every, None, None),
        P(every, None, None),
        P(),
        P(),
    )
    return jax.shard_map(
        body, mesh=mesh, in_specs=placed, out_specs=P(None, every), check_vma=False
    )
```

```python
import math

import jax
import jax.numpy as jnp
import numpy as np
from jax import lax
from jax.experimental import pallas as pl
from jax.experimental.pallas import tpu as pltpu
from jax.sharding import PartitionSpec as P

MESH = pl.DeviceIdType.MESH
D = 12288
HALF = 6144
EPSILON = 1e-05
THETA = 50000.0
MASKED = -1e30
WIN = 4096
HD = 128
COLS = 112
FFB = 136
OB = 96
NCOL = 3072
SCALE2 = 1.0 / math.sqrt(HD) / math.log(2.0)
F32 = jnp.float32
BF16 = jnp.bfloat16


def div(a, b):
    return lax.div(a, jnp.int32(b))


def rem(a, b):
    return lax.rem(a, jnp.int32(b))


NT = (((1,), (1,)), ((), ()))
TN = (((0,), (0,)), ((), ()))


def kernel(
    hidden, gain, qkv, out_w, gate, up, down, keys, values, pos_h, slots_h, freq_h, out,
    hid_v, gain_v, qkv_v, wo_v, gate_v, up_v, wd_v, k_v, v_v, normed_v,
    send1, recv1, qrow, cs_v, att_v, recv2, lhs_v, gu_send, gu_recv, act_v, acc_v,
    p1send, recvp1, p2send, recvp2, res_v, pos, slots, freq, bias_v, zsend, zrecv, zsum,
    load_sem, s1, r1, spre, rpre, s2, r2, s3, r3, s4, r4, sp1, rp1, sp2, rp2, sz, rz, sz2,
):
    s = lax.axis_index("side")
    g = lax.axis_index("grp")
    c = lax.axis_index("rep")
    z = div(g, 8)
    chip = rem(g, 8)
    j = 2 * g + c
    d16 = 2 * chip + c
    row_off = 64 * (rem(chip, 2))
    x, y = rem(chip, 4), div(chip, 4)
    odd = rem(x + y, 2)
    is_plane = (c == 0) | (odd == 1)
    is_line = c == div(z, 4)

    def load(src, dst, n):
        cp = pltpu.make_async_copy(src, dst, load_sem.at[n])
        cp.start()
        return cp

    quarter = D // 4
    hid_cp = [
        load(
            hidden.at[:, pl.ds(quarter * n, quarter)],
            hid_v.at[:, pl.ds(quarter * n, quarter)],
            n,
        )
        for n in range(4)
    ]
    gain_cp = load(gain, gain_v, 4)
    qkv_cp = load(qkv, qkv_v.at[pl.ds(0, COLS)], 5)

    barrier = pltpu.get_barrier_semaphore()

    def greet(side, grp, rep):
        pl.semaphore_signal(
            barrier, inc=1, device_id=(side, grp, rep), device_id_type=MESH
        )

    source = 8 * div(z, 7) + rem(z, 7)
    left = rem(z, 7)
    for cc in range(14):
        for near in (source, source + 1):
            greet(1 - s, div(near, 2), rem(near, 2))

            @pl.when(near != j)
            def _():
                greet(s, div(near, 2), rem(near, 2))

        left = left + 1
        wrap = left == 7
        source = source + jnp.where(wrap, 10, 9)
        left = jnp.where(wrap, 0, left)
    for o in range(16):
        i = rem(d16 + o, 16)
        greet(1 - s, 8 * z + div(i, 2), rem(i, 2))
        if o > 0:
            greet(s, 8 * z + div(i, 2), rem(i, 2))
    for o in range(1, 8):
        greet(s, 8 * rem(z + o, 8) + chip, c)

    gate_cp = load(gate, gate_v, 6)
    up_cp = load(up, up_v, 7)
    k_cp = load(keys, k_v, 8)
    v_cp = load(values, v_v, 9)
    own_cols = pl.ds(pl.multiple_of(NCOL * c, NCOL), NCOL)
    wo_cp = load(
        out_w.at[:, own_cols], wo_v.at[pl.ds(pl.multiple_of(row_off + OB * c, 32), OB)], 10
    )
    wd_cp = load(down.at[:, own_cols], wd_v.at[c], 11)
    pos_cp = load(pos_h, pos, 12)
    slots_cp = load(slots_h, slots, 13)
    freq_cp = load(freq_h, freq, 14)

    qkv_v[pl.ds(COLS, 16), :] = jnp.zeros((16, HALF), BF16)
    wo_v[pl.ds(pl.multiple_of(192 - 192 * (rem(chip, 2)), 64), 64), :] = jnp.zeros((64, NCOL), BF16)


    def chunk(i):
        return hid_v[:, pl.ds(pl.multiple_of(i * 128, 128), 128)].astype(F32)

    hid_cp[0].wait()
    pivot = jnp.sum(chunk(0), axis=1, keepdims=True) * (1.0 / 128)

    def moments(i, carry):
        one, two = carry
        d = chunk(i) - pivot
        return one + d, two + d * d

    carry = (jnp.zeros((64, 128), F32), jnp.zeros((64, 128), F32))
    for n in range(4):
        if n > 0:
            hid_cp[n].wait()
        carry = lax.fori_loop(24 * n, 24 * n + 24, moments, carry, unroll=8)
    shift = jnp.sum(carry[0], axis=1, keepdims=True) * (1.0 / D)
    mean = pivot + shift
    var = jnp.sum(carry[1], axis=1, keepdims=True) * (1.0 / D) - shift * shift
    rstd = lax.rsqrt(jnp.maximum(var, 0.0) + EPSILON)
    gain_cp.wait()
    qkv_cp.wait()

    term = jnp.zeros((64, 128), F32)
    for n in range(12):
        for w in range(4):
            at = 4 * n + w
            v = (chunk(s * 48 + at) - mean) * rstd * gain_v[pl.ds(s * 48 + at, 1), :]
            normed_v[:, 128 * at : 128 * at + 128] = v.astype(BF16)
        cols = slice(512 * n, 512 * n + 512)
        term = term + lax.dot_general(
            normed_v[:, cols], qkv_v[:, cols], NT, preferred_element_type=F32
        )
    m, t = div(j, 8), rem(j, 8)
    rolled = pltpu.roll(term, (128 - 16 * t) % 128, 1)
    lane = lax.broadcasted_iota(jnp.int32, (64, 128), 1)
    first = jnp.where(lane < COLS - 16 * t, rolled, 0.0)
    second = jnp.where(lane >= 128 - 16 * t, rolled, 0.0)
    for n in range(32):
        send1[n] = first[2 * n : 2 * n + 2]
        send1[32 + n] = second[2 * n : 2 * n + 2]

    mine = ((t <= 6) & (rem(7 * m + t, 8) == z)) | ((t >= 1) & (rem(7 * m + t + 7, 8) == z))
    edge = (t == 0) | (t == 7)
    pl.semaphore_wait(barrier, jnp.where(edge, 70, 102) - jnp.where(mine, 1, 0))

    valid = (t <= 6, t >= 1)
    for piece in range(2):
        q = jnp.maximum(7 * m + t - piece, 0)
        k, cc = rem(q, 8), div(q, 8)
        slot = jnp.minimum(cc, 13) * 4 + piece * 2 + s

        @pl.when(valid[piece])
        def _():
            def push(b, i):
                pltpu.make_async_remote_copy(
                    src_ref=send1.at[32 * piece + 16 * b + i],
                    dst_ref=recv1.at[slot],
                    send_sem=s1,
                    recv_sem=r1,
                    device_id=(b, 8 * k + div(i, 2), rem(i, 2)),
                    device_id_type=MESH,
                ).start()

            for o in range(16):
                i = rem(d16 + o, 16)
                push(1 - s, i)
                if o > 0:
                    push(s, i)

            @pl.when(k != z)
            def _():
                push(s, d16)

            @pl.when(k == z)
            def _():
                recv1[slot] = send1[32 * piece + s * 16 + d16]

    other_cols = pl.ds(pl.multiple_of(NCOL * (1 - c), NCOL), NCOL)
    sibling = (s, g, 1 - c)
    pre_out = pltpu.make_async_remote_copy(
        src_ref=out_w.at[:, other_cols],
        dst_ref=wo_v.at[pl.ds(pl.multiple_of(row_off + OB * c, 32), OB)],
        send_sem=spre.at[0],
        recv_sem=rpre.at[0],
        device_id=sibling,
        device_id_type=MESH,
    )
    pre_out.start()
    pre_down = pltpu.make_async_remote_copy(
        src_ref=down.at[:, other_cols],
        dst_ref=wd_v.at[c],
        send_sem=spre.at[1],
        recv_sem=rpre.at[1],
        device_id=sibling,
        device_id_type=MESH,
    )
    pre_down.start()

    gate_cp.wait()
    gu_send[:, 0:64] = lax.dot_general(
        gate_v[...], normed_v[...], NT, preferred_element_type=F32
    )
    up_cp.wait()
    gu_send[:, 64:128] = lax.dot_general(
        up_v[...], normed_v[...], NT, preferred_element_type=F32
    )
    gu = pltpu.make_async_remote_copy(
        src_ref=gu_send,
        dst_ref=gu_recv,
        send_sem=s3,
        recv_sem=r3,
        device_id=(1 - s, g, c),
        device_id_type=MESH,
    )
    gu.start()

    col0 = 48 * (128 * s + j)
    tile = jnp.minimum(div(col0, 128), 94)
    res_v[...] = hid_v[:, pl.ds(pl.multiple_of(tile * 128, 128), 256)].astype(F32).T
    res_off = pl.multiple_of(col0 - tile * 128, 16)

    lane1 = lax.broadcasted_iota(jnp.int32, (1, 128), 1)
    row0 = 32 * s + 2 * d16
    pos_cp.wait()
    slots_cp.wait()
    freq_cp.wait()
    for r in range(2):
        angle = pos[row0 + r].astype(F32) * freq[...]
        sine = jnp.sin(angle)
        cs_v[2 * r : 2 * r + 1, :] = jnp.cos(angle)
        cs_v[2 * r + 1 : 2 * r + 2, :] = jnp.where(lane1 < 64, -sine, sine)
    qrow[...] = jnp.zeros((2, 16, 128), F32)
    column = lax.broadcasted_iota(jnp.int32, (8, WIN), 1)
    for r in range(2):
        age = (slots[row0 + r] - column) & (WIN - 1)
        bias_v[r] = jnp.where((age > 0) & (age <= pos[row0 + r]), 0.0, MASKED)

    def wait_recv(src, dst, send, recv):
        pltpu.make_async_remote_copy(
            src_ref=src, dst_ref=dst, send_sem=send, recv_sem=recv,
            device_id=sibling, device_id_type=MESH,
        ).wait_recv()

    def wait_send(src, dst, send, recv):
        pltpu.make_async_remote_copy(
            src_ref=src, dst_ref=dst, send_sem=send, recv_sem=recv,
            device_id=sibling, device_id_type=MESH,
        ).wait_send()

    @pl.when(mine)
    def _():
        part = recv1.at[pl.ds(0, 55)]
        wait_recv(part, part, s1, r1)

    @pl.when(jnp.logical_not(mine))
    def _():
        wait_recv(recv1, recv1, s1, r1)

    for cc in range(14):
        both = (recv1[4 * cc] + recv1[4 * cc + 1]) + (recv1[4 * cc + 2] + recv1[4 * cc + 3])
        both = both.astype(BF16).astype(F32)
        qrow[0, cc : cc + 1, :] = both[0:1]
        qrow[1, cc : cc + 1, :] = both[1:2]

    k_cp.wait()
    v_cp.wait()
    for r in range(2):
        heads = qrow[r]
        turned = heads * cs_v[2 * r : 2 * r + 1, :] + pltpu.roll(heads, 64, 1) * cs_v[2 * r + 1 : 2 * r + 2, :]
        query = turned.astype(BF16)
        rounded = query.astype(F32)
        new_key = rounded[12:13]
        new_value = heads[13:14]
        fresh = jnp.sum(rounded * new_key, axis=1, keepdims=True)
        bias = bias_v[r]
        scores = lax.dot_general(query, k_v[r], NT, preferred_element_type=F32)
        scores = scores + jnp.concatenate([bias, bias], axis=0)
        highest = jnp.maximum(jnp.max(scores, axis=1, keepdims=True), fresh)
        weights = jnp.exp2((scores - highest) * SCALE2)
        own = jnp.exp2((fresh - highest) * SCALE2)
        denom = jnp.sum(weights, axis=1, keepdims=True) + own
        summed = jnp.dot(weights.astype(BF16), v_v[r], preferred_element_type=F32)
        own = own.astype(BF16).astype(F32)
        attended = ((summed + own * new_value) / denom).astype(BF16).astype(F32)
        for h in range(12):
            att_v[h, r : r + 1, :] = attended[h : h + 1]

    here = s * 16 + d16

    def spread_heads(b, i):
        u = div(i, 2)
        pltpu.make_async_remote_copy(
            src_ref=att_v.at[pl.ds(div(3 * u, 2), 2)],
            dst_ref=recv2.at[here],
            send_sem=s2,
            recv_sem=r2,
            device_id=(b, 8 * z + u, rem(i, 2)),
            device_id_type=MESH,
        ).start()

    for o in range(16):
        i = rem(d16 + o, 16)
        spread_heads(1 - s, i)
        if o > 0:
            spread_heads(s, i)
    recv2[here] = att_v[pl.ds(div(3 * chip, 2), 2)]

    gu.wait()
    both = gu_send[...] + gu_recv[...]
    lane136 = lax.broadcasted_iota(jnp.int32, (FFB, 128), 1)
    active = both / (1.0 + jnp.exp(-both)) * pltpu.roll(both, 64, 1)
    act_v[c] = jnp.where(lane136 < 64, active, 0.0).astype(BF16)
    act_cp = pltpu.make_async_remote_copy(
        src_ref=act_v.at[c],
        dst_ref=act_v.at[c],
        send_sem=s4,
        recv_sem=r4,
        device_id=sibling,
        device_id_type=MESH,
    )
    act_cp.start()
    wd_cp.wait()
    pre_down.wait()
    act_cp.wait()
    for n in range(6):
        cols = slice(512 * n, 512 * n + 512)
        acc_v[:, cols] = lax.dot_general(
            act_v[0, :, 0:64], wd_v[0, :, cols], TN, preferred_element_type=F32
        ) + lax.dot_general(
            act_v[1, :, 0:64], wd_v[1, :, cols], TN, preferred_element_type=F32
        )
    wo_cp.wait()
    pre_out.wait()

    most = recv2.at[pl.ds(0, 31)]
    wait_recv(most, most, s2, r2)
    for n in range(32):
        lhs_v[2 * n : 2 * n + 2, 0:128] = recv2[n, 0]
        lhs_v[2 * n : 2 * n + 2, 128:256] = recv2[n, 1]
    lhs = lhs_v[...].astype(BF16)
    for n in range(6):
        low = slice(256 * n, 256 * n + 256)
        high = slice(1536 + 256 * n, 1536 + 256 * n + 256)
        pa = jnp.dot(lhs, wo_v[:, low], preferred_element_type=F32) + acc_v[:, low]
        pb = jnp.dot(lhs, wo_v[:, high], preferred_element_type=F32) + acc_v[:, high]
        turned = jnp.concatenate([pa, pb], axis=0).T.astype(BF16)
        for w in range(16):
            at = 256 * n + 16 * w
            zl, rest = divmod(at, 768)
            dd, e = divmod(rest, 48)
            p1send[zl, dd, e : e + 16, :] = turned[16 * w : 16 * w + 16]

    def push_plane(chip_to, core):
        n = 2 * chip_to + core
        pltpu.make_async_remote_copy(
            src_ref=p1send.at[:, n],
            dst_ref=recvp1.at[d16],
            send_sem=sp1,
            recv_sem=rp1,
            device_id=(s, 8 * z + chip_to, core),
            device_id_type=MESH,
        ).start()

    def chip_at(dx, dy):
        return 4 * rem(y + dy, 2) + rem(x + dx, 4)

    steps = ((2, 1), (2, 0), (1, 1), (3, 1), (1, 0), (3, 0), (0, 1))
    for parity in range(2):

        @pl.when(odd == parity)
        def _():
            for dx, dy in steps:
                push_plane(chip_at(dx, dy), 0)
                if (parity + dx + dy) % 2 == 1:
                    push_plane(chip_at(dx, dy), 1)

    @pl.when(c == 1)
    def _():
        push_plane(chip, 0)

    @pl.when((c == 0) & (odd == 1))
    def _():
        push_plane(chip, 1)

    lane24 = lax.broadcasted_iota(jnp.int32, (24, 128), 1) < 64

    def folded(part):
        a, b = part[0:24], part[24:48]
        low = jnp.where(lane24, a, pltpu.roll(b, 64, 1)).astype(BF16)
        high = jnp.where(lane24, pltpu.roll(a, 64, 1), b).astype(BF16)
        return low, high

    for n in range(4):
        for zl in range(2):
            low, high = folded(p1send[zl, 8 * (n % 2) + 2 * n + 1].astype(F32))
            zsend[zl, n] = low
            zsend[2 + zl, n] = high
    for n in range(4):
        there = 4 * c + n

        @pl.when(there != z)
        def _():
            pltpu.make_async_remote_copy(
                src_ref=zsend.at[n],
                dst_ref=zrecv.at[z],
                send_sem=sz,
                recv_sem=rz,
                device_id=(s, 8 * there + chip, c),
                device_id_type=MESH,
            ).start()

    most1 = recvp1.at[pl.ds(0, 15)]
    most2 = recvp2.at[pl.ds(0, 7)]
    mostz = zrecv.at[pl.ds(0, 7)]

    @pl.when(is_plane)
    def _():
        recvp1[d16] = p1send[:, d16]
        wait_recv(most1, most1, sp1, rp1)
        for cs in range(2):
            for zl in range(2):
                part = recvp1[cs, zl].astype(F32)
                for p in range(1, 8):
                    part = part + recvp1[2 * p + cs, zl].astype(F32)
                low, high = folded(part)
                p2send[4 * cs + zl] = low
                p2send[4 * cs + 2 + zl] = high
        for o in (4, 3, 5, 2, 6, 1, 7):
            n = rem(z + o, 8)
            pltpu.make_async_remote_copy(
                src_ref=p2send.at[n],
                dst_ref=recvp2.at[z],
                send_sem=sp2,
                recv_sem=rp2,
                device_id=(s, 8 * n + chip, c),
                device_id_type=MESH,
            ).start()
        recvp2[z] = p2send[z]

    @pl.when(is_line)
    def _():
        zrecv[z] = zsend[rem(z, 4)]
        wait_recv(mostz, mostz, sz, rz)
        for n in range(4):
            part = zrecv[0, n].astype(F32)
            for p in range(1, 8):
                part = part + zrecv[p, n].astype(F32)
            zsum[n] = part.astype(BF16)
        for n in range(4):
            to = 4 * (n % 2) + n
            mine_too = (c == 1) & (chip == to)

            @pl.when(jnp.logical_not(mine_too))
            def _():
                pltpu.make_async_remote_copy(
                    src_ref=zsum.at[n],
                    dst_ref=recvp2.at[chip],
                    send_sem=sz2,
                    recv_sem=rp2,
                    device_id=(s, 8 * z + to, 1),
                    device_id_type=MESH,
                ).start()

            @pl.when(mine_too)
            def _():
                recvp2[chip] = zsum[n]

    eight = jnp.logical_not(is_plane) & (z < 4)

    @pl.when(eight)
    def _():
        wait_recv(recvp2, recvp2, sp2, rp2)

    @pl.when(jnp.logical_not(eight))
    def _():
        wait_recv(most2, most2, sp2, rp2)

    last = recvp2[0].astype(F32)
    for n in range(1, 8):
        last = last + recvp2[n].astype(F32)
    result = jnp.concatenate([last, pltpu.roll(last, 64, 1)], axis=0)[:, 0:64]
    out[...] = (result + res_v[pl.ds(res_off, 48), :]).astype(BF16)

    for count, when in (
        (64, jnp.logical_not(edge) & jnp.logical_not(mine)),
        (63, jnp.logical_not(edge) & mine),
        (32, edge & jnp.logical_not(mine)),
        (31, edge & mine),
    ):

        @pl.when(when)
        def _():
            part = send1.at[pl.ds(0, count)]
            wait_send(part, part, s1, r1)

    wait_send(most, most, s2, r2)
    for count, when in ((11, is_plane), (12, jnp.logical_not(is_plane))):

        @pl.when(when)
        def _():
            part = recvp1.at[pl.ds(0, count)]
            wait_send(part, part, sp1, rp1)

    for count, when in ((3, is_line), (4, jnp.logical_not(is_line))):

        @pl.when(when)
        def _():
            part = zrecv.at[pl.ds(0, count)]
            wait_send(part, part, sz, rz)

    @pl.when(is_plane)
    def _():
        wait_send(most2, most2, sp2, rp2)

    for count, when in ((4, is_plane), (3, jnp.logical_not(is_plane))):

        @pl.when(is_line & when)
        def _():
            part = recvp2.at[pl.ds(0, count)]
            wait_send(part, part, sz2, rp2)


def body(
    hidden, gain, qkv, out_w, gate, up, down, keys, values, positions, write_slots
):
    half = THETA ** (-2.0 * np.arange(64) / HD)
    freq = jnp.asarray(np.concatenate([half, half])[None, :].astype(np.float32))
    hbm = pl.BlockSpec(memory_space=pl.ANY)
    vmem = pl.BlockSpec(memory_space=pltpu.VMEM)
    dma = pltpu.SemaphoreType.DMA
    V = pltpu.VMEM
    result = pl.pallas_call(
        kernel,
        out_shape=pltpu.VMEM((48, 64), BF16),
        in_specs=[hbm] * 12,
        out_specs=vmem,
        scratch_shapes=[
            V((64, D), BF16),
            V((96, 128), F32),
            V((128, HALF), BF16),
            V((256, NCOL), BF16),
            V((FFB, HALF), BF16),
            V((FFB, HALF), BF16),
            V((2, FFB, NCOL), BF16),
            V((2, WIN, HD), BF16),
            V((2, WIN, HD), BF16),
            V((64, HALF), BF16),
            V((64, 2, 128), F32),
            V((56, 2, 128), F32),
            V((2, 16, 128), F32),
            V((8, 128), F32),
            V((12, 2, 128), F32),
            V((32, 2, 2, 128), F32),
            V((64, 256), F32),
            V((FFB, 128), F32),
            V((FFB, 128), F32),
            V((2, FFB, 128), BF16),
            V((64, NCOL), F32),
            V((2, 16, 48, 128), BF16),
            V((16, 2, 48, 128), BF16),
            V((8, 24, 128), BF16),
            V((8, 24, 128), BF16),
            V((256, 64), F32),
            pltpu.SMEM((64,), jnp.int32),
            pltpu.SMEM((64,), jnp.int32),
            V((1, 128), F32),
            V((2, 8, WIN), F32),
            V((4, 4, 24, 128), BF16),
            V((8, 4, 24, 128), BF16),
            V((4, 24, 128), BF16),
            dma((15,)),
            dma, dma,
            dma((2,)), dma((2,)),
            dma, dma, dma, dma, dma, dma, dma, dma, dma, dma, dma, dma, dma,
        ],
        compiler_params=pltpu.CompilerParams(
            collective_id=0, has_side_effects=True, vmem_limit_bytes=60 * 1024 * 1024
        ),
        name="layer",
    )(
        hidden,
        gain.reshape(96, 128),
        qkv.T,
        out_w,
        gate.T,
        up.T,
        down,
        keys,
        values,
        positions,
        write_slots,
        freq,
    )
    return result.T


def solution(mesh):
    side, grp, rep = mesh.axis_names
    inner = (grp, rep)
    every = (side, grp, rep)
    placed = (
        P(),
        P(),
        P(side, inner),
        P(inner, side),
        P(side, inner),
        P(side, inner),
        P(inner, side),
        P(every, None, None),
        P(every, None, None),
        P(),
        P(),
    )
    return jax.shard_map(
        body, mesh=mesh, in_specs=placed, out_specs=P(None, every), check_vma=False
    )
```

```python
import math

import jax
import jax.numpy as jnp
import numpy as np
from jax import lax
from jax.experimental import pallas as pl
from jax.experimental.pallas import tpu as pltpu
from jax.sharding import PartitionSpec as P

MESH = pl.DeviceIdType.MESH
D = 12288
HALF = 6144
EPSILON = 1e-05
THETA = 50000.0
MASKED = -1e30
WIN = 4096
HD = 128
COLS = 112
FFB = 136
OB = 96
NCOL = 3072
SCALE2 = 1.0 / math.sqrt(HD) / math.log(2.0)
F32 = jnp.float32
BF16 = jnp.bfloat16


def div(a, b):
    return lax.div(a, jnp.int32(b))


def rem(a, b):
    return lax.rem(a, jnp.int32(b))


NT = (((1,), (1,)), ((), ()))
TN = (((0,), (0,)), ((), ()))


def kernel(
    hidden, gain, qkv, out_w, gate, up, down, keys, values, pos_h, slots_h, freq_h, out,
    hid_v, gain_v, qkv_v, wo_v, gate_v, up_v, wd_v, k_v, v_v, normed_v,
    send1, recv1, qrow, cs_v, att_v, recv2, lhs_v, gu_send, gu_recv, act_v, acc_v,
    p1send, recvp1, p2send, recvp2, res_v, pos, slots, freq, bias_v, line1, zsend, zrecv, zsum, recvz2, score_v,
    load_sem, s1, r1, spre, rpre, s2, r2, s3, r3, s4, r4, sp1, rp1, sp2, rp2, sz, rz, sz2, rz2,
):
    s = lax.axis_index("side")
    g = lax.axis_index("grp")
    c = lax.axis_index("rep")
    z = div(g, 8)
    chip = rem(g, 8)
    j = 2 * g + c
    d16 = 2 * chip + c
    row_off = 64 * (rem(chip, 2))
    x, y = rem(chip, 4), div(chip, 4)
    is_line = c == div(z, 4)

    def load(src, dst, n):
        cp = pltpu.make_async_copy(src, dst, load_sem.at[n])
        cp.start()
        return cp

    quarter = D // 4
    hid_cp = [
        load(
            hidden.at[:, pl.ds(quarter * n, quarter)],
            hid_v.at[:, pl.ds(quarter * n, quarter)],
            n,
        )
        for n in range(4)
    ]
    gain_cp = load(gain, gain_v, 4)
    qkv_cp = load(qkv, qkv_v.at[pl.ds(0, COLS)], 5)

    barrier = pltpu.get_barrier_semaphore()

    def greet(side, grp, rep):
        pl.semaphore_signal(
            barrier, inc=1, device_id=(side, grp, rep), device_id_type=MESH
        )

    source = 8 * div(z, 7) + rem(z, 7)
    left = rem(z, 7)
    for cc in range(14):
        for near in (source, source + 1):
            greet(1 - s, div(near, 2), rem(near, 2))

            @pl.when(near != j)
            def _():
                greet(s, div(near, 2), rem(near, 2))

        left = left + 1
        wrap = left == 7
        source = source + jnp.where(wrap, 10, 9)
        left = jnp.where(wrap, 0, left)
    for o in range(16):
        i = rem(d16 + o, 16)
        greet(1 - s, 8 * z + div(i, 2), rem(i, 2))
        if o > 0:
            greet(s, 8 * z + div(i, 2), rem(i, 2))
    for o in range(1, 8):
        greet(s, 8 * rem(z + o, 8) + chip, c)

    gate_cp = load(gate, gate_v, 6)
    up_cp = load(up, up_v, 7)
    k_cp = load(keys, k_v, 8)
    v_cp = load(values, v_v, 9)
    own_cols = pl.ds(pl.multiple_of(NCOL * c, NCOL), NCOL)
    wo_cp = load(
        out_w.at[:, own_cols], wo_v.at[pl.ds(pl.multiple_of(row_off + OB * c, 32), OB)], 10
    )
    wd_cp = load(down.at[:, own_cols], wd_v.at[c], 11)
    pos_cp = load(pos_h, pos, 12)
    slots_cp = load(slots_h, slots, 13)
    freq_cp = load(freq_h, freq, 14)

    qkv_v[pl.ds(COLS, 16), :] = jnp.zeros((16, HALF), BF16)
    wo_v[pl.ds(pl.multiple_of(192 - 192 * (rem(chip, 2)), 64), 64), :] = jnp.zeros((64, NCOL), BF16)


    def chunk(i):
        return hid_v[:, pl.ds(pl.multiple_of(i * 128, 128), 128)].astype(F32)

    hid_cp[0].wait()
    pivot = jnp.sum(chunk(0), axis=1, keepdims=True) * (1.0 / 128)

    def moments(i, carry):
        one, two = carry
        d = chunk(i) - pivot
        return one + d, two + d * d

    carry = (jnp.zeros((64, 128), F32), jnp.zeros((64, 128), F32))
    for n in range(4):
        if n > 0:
            hid_cp[n].wait()
        carry = lax.fori_loop(24 * n, 24 * n + 24, moments, carry, unroll=8)
    shift = jnp.sum(carry[0], axis=1, keepdims=True) * (1.0 / D)
    mean = pivot + shift
    var = jnp.sum(carry[1], axis=1, keepdims=True) * (1.0 / D) - shift * shift
    rstd = lax.rsqrt(jnp.maximum(var, 0.0) + EPSILON)
    gain_cp.wait()
    qkv_cp.wait()

    term = jnp.zeros((64, 128), F32)
    for n in range(12):
        for w in range(4):
            at = 4 * n + w
            v = (chunk(s * 48 + at) - mean) * rstd * gain_v[pl.ds(s * 48 + at, 1), :]
            normed_v[:, 128 * at : 128 * at + 128] = v.astype(BF16)
        cols = slice(512 * n, 512 * n + 512)
        term = term + lax.dot_general(
            normed_v[:, cols], qkv_v[:, cols], NT, preferred_element_type=F32
        )
    m, t = div(j, 8), rem(j, 8)
    rolled = pltpu.roll(term, (128 - 16 * t) % 128, 1)
    lane = lax.broadcasted_iota(jnp.int32, (64, 128), 1)
    first = jnp.where(lane < COLS - 16 * t, rolled, 0.0)
    second = jnp.where(lane >= 128 - 16 * t, rolled, 0.0)
    for n in range(32):
        send1[n] = first[2 * n : 2 * n + 2]
        send1[32 + n] = second[2 * n : 2 * n + 2]

    mine = ((t <= 6) & (rem(7 * m + t, 8) == z)) | ((t >= 1) & (rem(7 * m + t + 7, 8) == z))
    edge = (t == 0) | (t == 7)
    pl.semaphore_wait(barrier, jnp.where(edge, 70, 102) - jnp.where(mine, 1, 0))

    valid = (t <= 6, t >= 1)
    for piece in range(2):
        q = jnp.maximum(7 * m + t - piece, 0)
        k, cc = rem(q, 8), div(q, 8)
        slot = jnp.minimum(cc, 13) * 4 + piece * 2 + s

        @pl.when(valid[piece])
        def _():
            def push(b, i):
                pltpu.make_async_remote_copy(
                    src_ref=send1.at[32 * piece + 16 * b + i],
                    dst_ref=recv1.at[slot],
                    send_sem=s1,
                    recv_sem=r1,
                    device_id=(b, 8 * k + div(i, 2), rem(i, 2)),
                    device_id_type=MESH,
                ).start()

            for o in range(16):
                i = rem(d16 + o, 16)
                push(1 - s, i)
                if o > 0:
                    push(s, i)

            @pl.when(k != z)
            def _():
                push(s, d16)

            @pl.when(k == z)
            def _():
                recv1[slot] = send1[32 * piece + s * 16 + d16]

    other_cols = pl.ds(pl.multiple_of(NCOL * (1 - c), NCOL), NCOL)
    sibling = (s, g, 1 - c)
    pre_out = pltpu.make_async_remote_copy(
        src_ref=out_w.at[:, other_cols],
        dst_ref=wo_v.at[pl.ds(pl.multiple_of(row_off + OB * c, 32), OB)],
        send_sem=spre.at[0],
        recv_sem=rpre.at[0],
        device_id=sibling,
        device_id_type=MESH,
    )
    pre_out.start()
    pre_down = pltpu.make_async_remote_copy(
        src_ref=down.at[:, other_cols],
        dst_ref=wd_v.at[c],
        send_sem=spre.at[1],
        recv_sem=rpre.at[1],
        device_id=sibling,
        device_id_type=MESH,
    )
    pre_down.start()

    gate_cp.wait()
    gu_send[:, 0:64] = lax.dot_general(
        gate_v[...], normed_v[...], NT, preferred_element_type=F32
    )
    up_cp.wait()
    gu_send[:, 64:128] = lax.dot_general(
        up_v[...], normed_v[...], NT, preferred_element_type=F32
    )
    gu = pltpu.make_async_remote_copy(
        src_ref=gu_send,
        dst_ref=gu_recv,
        send_sem=s3,
        recv_sem=r3,
        device_id=(1 - s, g, c),
        device_id_type=MESH,
    )
    gu.start()

    col0 = 48 * (128 * s + j)
    tile = jnp.minimum(div(col0, 128), 94)
    res_v[...] = hid_v[:, pl.ds(pl.multiple_of(tile * 128, 128), 256)].astype(F32).T
    res_off = pl.multiple_of(col0 - tile * 128, 16)

    lane1 = lax.broadcasted_iota(jnp.int32, (1, 128), 1)
    row0 = 32 * s + 2 * d16
    pos_cp.wait()
    slots_cp.wait()
    freq_cp.wait()
    for r in range(2):
        angle = pos[row0 + r].astype(F32) * freq[...]
        sine = jnp.sin(angle)
        cs_v[2 * r : 2 * r + 1, :] = jnp.cos(angle)
        cs_v[2 * r + 1 : 2 * r + 2, :] = jnp.where(lane1 < 64, -sine, sine)
    qrow[...] = jnp.zeros((2, 16, 128), F32)
    column = lax.broadcasted_iota(jnp.int32, (8, WIN), 1)
    for r in range(2):
        age = (slots[row0 + r] - column) & (WIN - 1)
        bias_v[r] = jnp.where((age > 0) & (age <= pos[row0 + r]), 0.0, MASKED)

    def wait_recv(src, dst, send, recv):
        pltpu.make_async_remote_copy(
            src_ref=src, dst_ref=dst, send_sem=send, recv_sem=recv,
            device_id=sibling, device_id_type=MESH,
        ).wait_recv()

    def wait_send(src, dst, send, recv):
        pltpu.make_async_remote_copy(
            src_ref=src, dst_ref=dst, send_sem=send, recv_sem=recv,
            device_id=sibling, device_id_type=MESH,
        ).wait_send()

    @pl.when(mine)
    def _():
        part = recv1.at[pl.ds(0, 55)]
        wait_recv(part, part, s1, r1)

    @pl.when(jnp.logical_not(mine))
    def _():
        wait_recv(recv1, recv1, s1, r1)

    for cc in range(14):
        both = (recv1[4 * cc] + recv1[4 * cc + 1]) + (recv1[4 * cc + 2] + recv1[4 * cc + 3])
        both = both.astype(BF16).astype(F32)
        qrow[0, cc : cc + 1, :] = both[0:1]
        qrow[1, cc : cc + 1, :] = both[1:2]

    k_cp.wait()
    v_cp.wait()
    rows = []
    for r in range(2):
        heads = qrow[r]
        turned = heads * cs_v[2 * r : 2 * r + 1, :] + pltpu.roll(heads, 64, 1) * cs_v[2 * r + 1 : 2 * r + 2, :]
        query = turned.astype(BF16)
        rounded = query.astype(F32)
        fresh = jnp.sum(rounded * rounded[12:13], axis=1, keepdims=True)
        highest = fresh
        for n in range(4):
            part = slice(1024 * n, 1024 * n + 1024)
            bias = bias_v[r, :, part]
            scores = lax.dot_general(query, k_v[r, part, :], NT, preferred_element_type=F32)
            scores = scores + jnp.concatenate([bias, bias], axis=0)
            score_v[r, :, part] = scores
            highest = jnp.maximum(highest, jnp.max(scores, axis=1, keepdims=True))
        rows.append((heads[13:14], fresh, highest))
    for r in range(2):
        new_value, fresh, highest = rows[r]
        own = jnp.exp2((fresh - highest) * SCALE2)
        denom = own
        summed = own.astype(BF16).astype(F32) * new_value
        for n in range(4):
            part = slice(1024 * n, 1024 * n + 1024)
            weights = jnp.exp2((score_v[r, :, part] - highest) * SCALE2)
            denom = denom + jnp.sum(weights, axis=1, keepdims=True)
            summed = summed + jnp.dot(
                weights.astype(BF16), v_v[r, part, :], preferred_element_type=F32
            )
        attended = (summed / denom).astype(BF16).astype(F32)
        for h in range(12):
            att_v[h, r : r + 1, :] = attended[h : h + 1]

    here = s * 16 + d16

    def spread_heads(b, i):
        u = div(i, 2)
        pltpu.make_async_remote_copy(
            src_ref=att_v.at[pl.ds(div(3 * u, 2), 2)],
            dst_ref=recv2.at[here],
            send_sem=s2,
            recv_sem=r2,
            device_id=(b, 8 * z + u, rem(i, 2)),
            device_id_type=MESH,
        ).start()

    for o in range(16):
        i = rem(d16 + o, 16)
        spread_heads(1 - s, i)
        if o > 0:
            spread_heads(s, i)
    recv2[here] = att_v[pl.ds(div(3 * chip, 2), 2)]

    gu.wait()
    both = gu_send[...] + gu_recv[...]
    lane136 = lax.broadcasted_iota(jnp.int32, (FFB, 128), 1)
    active = both / (1.0 + jnp.exp(-both)) * pltpu.roll(both, 64, 1)
    act_v[c] = jnp.where(lane136 < 64, active, 0.0).astype(BF16)
    act_cp = pltpu.make_async_remote_copy(
        src_ref=act_v.at[c],
        dst_ref=act_v.at[c],
        send_sem=s4,
        recv_sem=r4,
        device_id=sibling,
        device_id_type=MESH,
    )
    act_cp.start()
    wd_cp.wait()
    pre_down.wait()
    act_cp.wait()
    for n in range(6):
        cols = slice(512 * n, 512 * n + 512)
        acc_v[:, cols] = lax.dot_general(
            act_v[0, :, 0:64], wd_v[0, :, cols], TN, preferred_element_type=F32
        ) + lax.dot_general(
            act_v[1, :, 0:64], wd_v[1, :, cols], TN, preferred_element_type=F32
        )
    wo_cp.wait()
    pre_out.wait()

    most = recv2.at[pl.ds(0, 31)]
    wait_recv(most, most, s2, r2)
    for n in range(32):
        lhs_v[2 * n : 2 * n + 2, 0:128] = recv2[n, 0]
        lhs_v[2 * n : 2 * n + 2, 128:256] = recv2[n, 1]
    lhs = lhs_v[...].astype(BF16)
    for n in range(6):
        low = slice(256 * n, 256 * n + 256)
        high = slice(1536 + 256 * n, 1536 + 256 * n + 256)
        pa = jnp.dot(lhs, wo_v[:, low], preferred_element_type=F32) + acc_v[:, low]
        pb = jnp.dot(lhs, wo_v[:, high], preferred_element_type=F32) + acc_v[:, high]
        turned = jnp.concatenate([pa, pb], axis=0).T.astype(BF16)
        for w in range(16):
            at = 256 * n + 16 * w
            zl, rest = divmod(at, 768)
            dd, e = divmod(rest, 48)
            if e == 0:
                line1[zl, dd] = turned[16 * w : 16 * w + 16]
            else:
                p1send[zl, dd, e - 16 : e, :] = turned[16 * w : 16 * w + 16]

    def push_plane(chip_to, core):
        n = 2 * chip_to + core
        pltpu.make_async_remote_copy(
            src_ref=p1send.at[:, n],
            dst_ref=recvp1.at[d16],
            send_sem=sp1,
            recv_sem=rp1,
            device_id=(s, 8 * z + chip_to, core),
            device_id_type=MESH,
        ).start()

    for dx, dy in ((2, 1), (2, 0), (1, 1), (3, 1), (1, 0), (3, 0), (0, 1)):
        chip_to = 4 * rem(y + dy, 2) + rem(x + dx, 4)
        push_plane(chip_to, 0)
        push_plane(chip_to, 1)
    push_plane(chip, 1 - c)

    def folded(part):
        half = part.shape[0] // 2
        left = lax.broadcasted_iota(jnp.int32, (half, 128), 1) < 64
        a, b = part[:half], part[half:]
        low = jnp.where(left, a, pltpu.roll(b, 64, 1)).astype(BF16)
        high = jnp.where(left, pltpu.roll(a, 64, 1), b).astype(BF16)
        return low, high

    for n in range(16):
        for zl in range(2):
            low, high = folded(line1[zl, n].astype(F32))
            zsend[zl, n] = low
            zsend[2 + zl, n] = high
    for n in range(4):
        there = 4 * c + n

        @pl.when(there != z)
        def _():
            pltpu.make_async_remote_copy(
                src_ref=zsend.at[n],
                dst_ref=zrecv.at[z],
                send_sem=sz,
                recv_sem=rz,
                device_id=(s, 8 * there + chip, c),
                device_id_type=MESH,
            ).start()

    most1 = recvp1.at[pl.ds(0, 15)]
    most2 = recvp2.at[pl.ds(0, 7)]
    mostz = zrecv.at[pl.ds(0, 7)]
    recvp1[d16] = p1send[:, d16]
    wait_recv(most1, most1, sp1, rp1)
    for cs in range(2):
        for zl in range(2):
            part = recvp1[cs, zl].astype(F32)
            for p in range(1, 8):
                part = part + recvp1[2 * p + cs, zl].astype(F32)
            low, high = folded(part)
            p2send[4 * cs + zl] = low
            p2send[4 * cs + 2 + zl] = high
    for o in (4, 3, 5, 2, 6, 1, 7):
        n = rem(z + o, 8)
        pltpu.make_async_remote_copy(
            src_ref=p2send.at[n],
            dst_ref=recvp2.at[z],
            send_sem=sp2,
            recv_sem=rp2,
            device_id=(s, 8 * n + chip, c),
            device_id_type=MESH,
        ).start()
    recvp2[z] = p2send[z]

    @pl.when(is_line)
    def _():
        zrecv[z] = zsend[rem(z, 4)]
        wait_recv(mostz, mostz, sz, rz)
        for n in range(16):
            part = zrecv[0, n].astype(F32)
            for p in range(1, 8):
                part = part + zrecv[p, n].astype(F32)
            zsum[n] = part.astype(BF16)
        for o in range(1, 16):
            n = rem(d16 + o, 16)
            pltpu.make_async_remote_copy(
                src_ref=zsum.at[n],
                dst_ref=recvz2.at[chip],
                send_sem=sz2,
                recv_sem=rz2,
                device_id=(s, 8 * z + div(n, 2), rem(n, 2)),
                device_id_type=MESH,
            ).start()
        recvz2[chip] = zsum[d16]
        seven = recvz2.at[pl.ds(0, 7)]
        wait_recv(seven, seven, sz2, rz2)

    @pl.when(jnp.logical_not(is_line))
    def _():
        wait_recv(recvz2, recvz2, sz2, rz2)

    wait_recv(most2, most2, sp2, rp2)
    last = recvp2[0].astype(F32)
    for n in range(1, 8):
        last = last + recvp2[n].astype(F32)
    line = recvz2[0].astype(F32)
    for n in range(1, 8):
        line = line + recvz2[n].astype(F32)
    result = jnp.concatenate(
        [line, pltpu.roll(line, 64, 1), last, pltpu.roll(last, 64, 1)], axis=0
    )[:, 0:64]
    out[...] = (result + res_v[pl.ds(res_off, 48), :]).astype(BF16)

    for count, when in (
        (64, jnp.logical_not(edge) & jnp.logical_not(mine)),
        (63, jnp.logical_not(edge) & mine),
        (32, edge & jnp.logical_not(mine)),
        (31, edge & mine),
    ):

        @pl.when(when)
        def _():
            part = send1.at[pl.ds(0, count)]
            wait_send(part, part, s1, r1)

    wait_send(most, most, s2, r2)
    wait_send(most1, most1, sp1, rp1)
    wait_send(most2, most2, sp2, rp2)
    for count, when in ((3, is_line), (4, jnp.logical_not(is_line))):

        @pl.when(when)
        def _():
            part = zrecv.at[pl.ds(0, count)]
            wait_send(part, part, sz, rz)

    @pl.when(is_line)
    def _():
        part = zsum.at[pl.ds(0, 15)]
        wait_send(part, part, sz2, rz2)


def body(
    hidden, gain, qkv, out_w, gate, up, down, keys, values, positions, write_slots
):
    half = THETA ** (-2.0 * np.arange(64) / HD)
    freq = jnp.asarray(np.concatenate([half, half])[None, :].astype(np.float32))
    hbm = pl.BlockSpec(memory_space=pl.ANY)
    vmem = pl.BlockSpec(memory_space=pltpu.VMEM)
    dma = pltpu.SemaphoreType.DMA
    V = pltpu.VMEM
    result = pl.pallas_call(
        kernel,
        out_shape=pltpu.VMEM((48, 64), BF16),
        in_specs=[hbm] * 12,
        out_specs=vmem,
        scratch_shapes=[
            V((64, D), BF16),
            V((96, 128), F32),
            V((128, HALF), BF16),
            V((256, NCOL), BF16),
            V((FFB, HALF), BF16),
            V((FFB, HALF), BF16),
            V((2, FFB, NCOL), BF16),
            V((2, WIN, HD), BF16),
            V((2, WIN, HD), BF16),
            V((64, HALF), BF16),
            V((64, 2, 128), F32),
            V((56, 2, 128), F32),
            V((2, 16, 128), F32),
            V((8, 128), F32),
            V((12, 2, 128), F32),
            V((32, 2, 2, 128), F32),
            V((64, 256), F32),
            V((FFB, 128), F32),
            V((FFB, 128), F32),
            V((2, FFB, 128), BF16),
            V((64, NCOL), F32),
            V((2, 16, 32, 128), BF16),
            V((16, 2, 32, 128), BF16),
            V((8, 16, 128), BF16),
            V((8, 16, 128), BF16),
            V((256, 64), F32),
            pltpu.SMEM((64,), jnp.int32),
            pltpu.SMEM((64,), jnp.int32),
            V((1, 128), F32),
            V((2, 8, WIN), F32),
            V((2, 16, 16, 128), BF16),
            V((4, 16, 8, 128), BF16),
            V((8, 16, 8, 128), BF16),
            V((16, 8, 128), BF16),
            V((8, 8, 128), BF16),
            V((2, 16, WIN), F32),
            dma((15,)),
            dma, dma,
            dma((2,)), dma((2,)),
            dma, dma, dma, dma, dma, dma, dma, dma, dma, dma, dma, dma, dma, dma,
        ],
        compiler_params=pltpu.CompilerParams(
            collective_id=0, has_side_effects=True, vmem_limit_bytes=60 * 1024 * 1024
        ),
        name="layer",
    )(
        hidden,
        gain.reshape(96, 128),
        qkv.T,
        out_w,
        gate.T,
        up.T,
        down,
        keys,
        values,
        positions,
        write_slots,
        freq,
    )
    return result.T


def solution(mesh):
    side, grp, rep = mesh.axis_names
    inner = (grp, rep)
    every = (side, grp, rep)
    placed = (
        P(),
        P(),
        P(side, inner),
        P(inner, side),
        P(side, inner),
        P(side, inner),
        P(inner, side),
        P(every, None, None),
        P(every, None, None),
        P(),
        P(),
    )
    return jax.shard_map(
        body, mesh=mesh, in_specs=placed, out_specs=P(None, every), check_vma=False
    )
```

```python
import math

import jax
import jax.numpy as jnp
import numpy as np
from jax import lax
from jax.experimental import pallas as pl
from jax.experimental.pallas import tpu as pltpu
from jax.sharding import PartitionSpec as P

MESH = pl.DeviceIdType.MESH
D = 12288
HALF = 6144
EPSILON = 1e-05
THETA = 50000.0
MASKED = -1e30
WIN = 4096
HD = 128
COLS = 112
FFB = 136
OB = 96
NCOL = 3072
PARTS = 8
SCALE2 = 1.0 / math.sqrt(HD) / math.log(2.0)
F32 = jnp.float32
BF16 = jnp.bfloat16


def div(a, b):
    return lax.div(a, jnp.int32(b))


def rem(a, b):
    return lax.rem(a, jnp.int32(b))


NT = (((1,), (1,)), ((), ()))
TN = (((0,), (0,)), ((), ()))


def kernel(
    hidden, gain, qkv, out_w, gate, up, down, keys, values, pos_h, slots_h, freq_h, out,
    hid_v, gain_v, qkv_v, wo_v, gate_v, up_v, wd_v, k_v, v_v, normed_v,
    send1, recv1, qrow, cs_v, att_v, recv2, lhs_v, gu_send, gu_recv, act_v, acc_v,
    p1send, recvp1, p2send, recvp2, res_v, pos, slots, freq, bias_v, line1, zsend, zrecv, zsum, recvz2, score_v, kt_v,
    load_sem, s1, r1, spre, rpre, s2, r2, s3, r3, s4, r4, sp1, rp1, sp2, rp2, sz, rz, sz2, rz2,
):
    s = lax.axis_index("side")
    g = lax.axis_index("grp")
    c = lax.axis_index("rep")
    z = div(g, 8)
    chip = rem(g, 8)
    j = 2 * g + c
    d16 = 2 * chip + c
    row_off = 64 * (rem(chip, 2))
    x, y = rem(chip, 4), div(chip, 4)
    is_line = c == div(z, 4)

    def load(src, dst, n):
        cp = pltpu.make_async_copy(src, dst, load_sem.at[n])
        cp.start()
        return cp

    quarter = D // 4
    hid_cp = [
        load(
            hidden.at[:, pl.ds(quarter * n, quarter)],
            hid_v.at[:, pl.ds(quarter * n, quarter)],
            n,
        )
        for n in range(4)
    ]
    gain_cp = load(gain, gain_v, 4)
    qkv_cp = load(qkv, qkv_v.at[pl.ds(0, COLS)], 5)

    barrier = pltpu.get_barrier_semaphore()

    def greet(side, grp, rep):
        pl.semaphore_signal(
            barrier, inc=1, device_id=(side, grp, rep), device_id_type=MESH
        )

    source = 8 * div(z, 7) + rem(z, 7)
    left = rem(z, 7)
    for cc in range(14):
        for near in (source, source + 1):
            greet(1 - s, div(near, 2), rem(near, 2))

            @pl.when(near != j)
            def _():
                greet(s, div(near, 2), rem(near, 2))

        left = left + 1
        wrap = left == 7
        source = source + jnp.where(wrap, 10, 9)
        left = jnp.where(wrap, 0, left)
    for o in range(16):
        i = rem(d16 + o, 16)
        greet(1 - s, 8 * z + div(i, 2), rem(i, 2))
        if o > 0:
            greet(s, 8 * z + div(i, 2), rem(i, 2))
    for o in range(1, 8):
        greet(s, 8 * rem(z + o, 8) + chip, c)

    gate_cp = load(gate, gate_v, 6)
    up_cp = load(up, up_v, 7)
    k_cp = load(keys, k_v, 8)
    kv_cp = [
        load(values.at[r], v_v.at[:, pl.ds(HD * r, HD)], 15 + r) for r in range(2)
    ]
    own_cols = pl.ds(pl.multiple_of(NCOL * c, NCOL), NCOL)
    wo_cp = load(
        out_w.at[:, own_cols], wo_v.at[pl.ds(pl.multiple_of(row_off + OB * c, 32), OB)], 10
    )
    wd_cp = load(down.at[:, own_cols], wd_v.at[c], 11)
    pos_cp = load(pos_h, pos, 12)
    slots_cp = load(slots_h, slots, 13)
    freq_cp = load(freq_h, freq, 14)

    qkv_v[pl.ds(COLS, 16), :] = jnp.zeros((16, HALF), BF16)
    wo_v[pl.ds(pl.multiple_of(192 - 192 * (rem(chip, 2)), 64), 64), :] = jnp.zeros((64, NCOL), BF16)


    def chunk(i):
        return hid_v[:, pl.ds(pl.multiple_of(i * 128, 128), 128)].astype(F32)

    hid_cp[0].wait()
    pivot = jnp.sum(chunk(0), axis=1, keepdims=True) * (1.0 / 128)

    def moments(i, carry):
        one, two = carry
        d = chunk(i) - pivot
        return one + d, two + d * d

    carry = (jnp.zeros((64, 128), F32), jnp.zeros((64, 128), F32))
    for n in range(4):
        if n > 0:
            hid_cp[n].wait()
        carry = lax.fori_loop(24 * n, 24 * n + 24, moments, carry, unroll=8)
    shift = jnp.sum(carry[0], axis=1, keepdims=True) * (1.0 / D)
    mean = pivot + shift
    var = jnp.sum(carry[1], axis=1, keepdims=True) * (1.0 / D) - shift * shift
    rstd = lax.rsqrt(jnp.maximum(var, 0.0) + EPSILON)
    gain_cp.wait()
    qkv_cp.wait()

    term = jnp.zeros((64, 128), F32)
    for n in range(12):
        for w in range(4):
            at = 4 * n + w
            v = (chunk(s * 48 + at) - mean) * rstd * gain_v[pl.ds(s * 48 + at, 1), :]
            normed_v[:, 128 * at : 128 * at + 128] = v.astype(BF16)
        cols = slice(512 * n, 512 * n + 512)
        term = term + lax.dot_general(
            normed_v[:, cols], qkv_v[:, cols], NT, preferred_element_type=F32
        )
    m, t = div(j, 8), rem(j, 8)
    rolled = pltpu.roll(term, (128 - 16 * t) % 128, 1)
    lane = lax.broadcasted_iota(jnp.int32, (64, 128), 1)
    first = jnp.where(lane < COLS - 16 * t, rolled, 0.0)
    second = jnp.where(lane >= 128 - 16 * t, rolled, 0.0)
    for n in range(32):
        send1[n] = first[2 * n : 2 * n + 2]
        send1[32 + n] = second[2 * n : 2 * n + 2]

    mine = ((t <= 6) & (rem(7 * m + t, 8) == z)) | ((t >= 1) & (rem(7 * m + t + 7, 8) == z))
    edge = (t == 0) | (t == 7)
    pl.semaphore_wait(barrier, jnp.where(edge, 70, 102) - jnp.where(mine, 1, 0))

    valid = (t <= 6, t >= 1)
    for piece in range(2):
        q = jnp.maximum(7 * m + t - piece, 0)
        k, cc = rem(q, 8), div(q, 8)
        slot = jnp.minimum(cc, 13) * 4 + piece * 2 + s

        @pl.when(valid[piece])
        def _():
            def push(b, i):
                pltpu.make_async_remote_copy(
                    src_ref=send1.at[32 * piece + 16 * b + i],
                    dst_ref=recv1.at[slot],
                    send_sem=s1,
                    recv_sem=r1,
                    device_id=(b, 8 * k + div(i, 2), rem(i, 2)),
                    device_id_type=MESH,
                ).start()

            for o in range(16):
                i = rem(d16 + o, 16)
                push(1 - s, i)
                if o > 0:
                    push(s, i)

            @pl.when(k != z)
            def _():
                push(s, d16)

            @pl.when(k == z)
            def _():
                recv1[slot] = send1[32 * piece + s * 16 + d16]

    other_cols = pl.ds(pl.multiple_of(NCOL * (1 - c), NCOL), NCOL)
    sibling = (s, g, 1 - c)
    pre_out = pltpu.make_async_remote_copy(
        src_ref=out_w.at[:, other_cols],
        dst_ref=wo_v.at[pl.ds(pl.multiple_of(row_off + OB * c, 32), OB)],
        send_sem=spre.at[0],
        recv_sem=rpre.at[0],
        device_id=sibling,
        device_id_type=MESH,
    )
    pre_out.start()
    pre_down = pltpu.make_async_remote_copy(
        src_ref=down.at[:, other_cols],
        dst_ref=wd_v.at[c],
        send_sem=spre.at[1],
        recv_sem=rpre.at[1],
        device_id=sibling,
        device_id_type=MESH,
    )
    pre_down.start()

    gate_cp.wait()
    gu_send[:, 0:64] = lax.dot_general(
        gate_v[...], normed_v[...], NT, preferred_element_type=F32
    )
    up_cp.wait()
    gu_send[:, 64:128] = lax.dot_general(
        up_v[...], normed_v[...], NT, preferred_element_type=F32
    )
    gu = pltpu.make_async_remote_copy(
        src_ref=gu_send,
        dst_ref=gu_recv,
        send_sem=s3,
        recv_sem=r3,
        device_id=(1 - s, g, c),
        device_id_type=MESH,
    )
    gu.start()

    col0 = 48 * (128 * s + j)
    tile = jnp.minimum(div(col0, 128), 94)
    res_v[...] = hid_v[:, pl.ds(pl.multiple_of(tile * 128, 128), 256)].astype(F32).T
    res_off = pl.multiple_of(col0 - tile * 128, 16)

    lane1 = lax.broadcasted_iota(jnp.int32, (1, 128), 1)
    row0 = 32 * s + 2 * d16
    pos_cp.wait()
    slots_cp.wait()
    freq_cp.wait()
    for r in range(2):
        angle = pos[row0 + r].astype(F32) * freq[...]
        sine = jnp.sin(angle)
        cs_v[2 * r : 2 * r + 1, :] = jnp.cos(angle)
        cs_v[2 * r + 1 : 2 * r + 2, :] = jnp.where(lane1 < 64, -sine, sine)
    qrow[...] = jnp.zeros((2, 16, 128), F32)
    k_cp.wait()
    for r in range(2):
        for n in range(8):
            part = slice(512 * n, 512 * n + 512)
            kt_v[HD * r : HD * r + HD, part] = k_v[r, part, :].T
    column = lax.broadcasted_iota(jnp.int32, (8, WIN), 1)
    for r in range(2):
        age = (slots[row0 + r] - column) & (WIN - 1)
        bias_v[r] = jnp.where((age > 0) & (age <= pos[row0 + r]), 0.0, MASKED)

    def wait_recv(src, dst, send, recv):
        pltpu.make_async_remote_copy(
            src_ref=src, dst_ref=dst, send_sem=send, recv_sem=recv,
            device_id=sibling, device_id_type=MESH,
        ).wait_recv()

    def wait_send(src, dst, send, recv):
        pltpu.make_async_remote_copy(
            src_ref=src, dst_ref=dst, send_sem=send, recv_sem=recv,
            device_id=sibling, device_id_type=MESH,
        ).wait_send()

    @pl.when(mine)
    def _():
        part = recv1.at[pl.ds(0, 55)]
        wait_recv(part, part, s1, r1)

    @pl.when(jnp.logical_not(mine))
    def _():
        wait_recv(recv1, recv1, s1, r1)

    for cc in range(14):
        both = (recv1[4 * cc] + recv1[4 * cc + 1]) + (recv1[4 * cc + 2] + recv1[4 * cc + 3])
        both = both.astype(BF16).astype(F32)
        qrow[0, cc : cc + 1, :] = both[0:1]
        qrow[1, cc : cc + 1, :] = both[1:2]

    for cp in kv_cp:
        cp.wait()
    queries, news, fresh = [], [], []
    blank = jnp.zeros((16, 128), BF16)
    for r in range(2):
        heads = qrow[r]
        turned = heads * cs_v[2 * r : 2 * r + 1, :] + pltpu.roll(heads, 64, 1) * cs_v[2 * r + 1 : 2 * r + 2, :]
        query = turned.astype(BF16)
        rounded = query.astype(F32)
        fresh.append(jnp.sum(rounded * rounded[12:13], axis=1, keepdims=True))
        queries.append(jnp.concatenate([query, blank] if r == 0 else [blank, query], axis=1))
        news.append(heads[13:14])
    query = jnp.concatenate(queries, axis=0)
    fresh = jnp.concatenate(fresh, axis=0)
    highest = fresh
    for n in range(PARTS):
        part = slice(WIN // PARTS * n, WIN // PARTS * (n + 1))
        scores = jnp.dot(query, kt_v[:, part], preferred_element_type=F32)
        bias = [bias_v[r, :, part] for r in (0, 0, 1, 1)]
        scores = scores + jnp.concatenate(bias, axis=0)
        score_v[:, part] = scores
        highest = jnp.maximum(highest, jnp.max(scores, axis=1, keepdims=True))
    own = jnp.exp2((fresh - highest) * SCALE2)
    denom = own
    summed = jnp.zeros((32, 256), F32)
    for n in range(PARTS):
        part = slice(WIN // PARTS * n, WIN // PARTS * (n + 1))
        weights = jnp.exp2((score_v[:, part] - highest) * SCALE2)
        denom = denom + jnp.sum(weights, axis=1, keepdims=True)
        summed = summed + jnp.dot(
            weights.astype(BF16), v_v[part, :], preferred_element_type=F32
        )
    own = own.astype(BF16).astype(F32)
    attended = [
        (summed[16 * r : 16 * r + 16, HD * r : HD * r + HD] + own[16 * r : 16 * r + 16] * news[r])
        / denom[16 * r : 16 * r + 16]
        for r in range(2)
    ]
    for h in range(12):
        att_v[h] = jnp.concatenate(
            [attended[0][h : h + 1], attended[1][h : h + 1]], axis=0
        ).astype(BF16)

    here = s * 16 + d16

    def spread_heads(b, i):
        u = div(i, 2)
        pltpu.make_async_remote_copy(
            src_ref=att_v.at[pl.ds(div(3 * u, 2), 2)],
            dst_ref=recv2.at[here],
            send_sem=s2,
            recv_sem=r2,
            device_id=(b, 8 * z + u, rem(i, 2)),
            device_id_type=MESH,
        ).start()

    for dx in (2, 1, 3, 0):
        for side, dy in ((1 - s, 0), (1 - s, 1), (s, 1), (s, 0)):
            i = 2 * (4 * rem(y + dy, 2) + rem(x + dx, 4))
            if dx == 0 and dy == 0 and side is s:
                spread_heads(s, i + 1 - c)
            else:
                spread_heads(side, i)
                spread_heads(side, i + 1)
    recv2[here] = att_v[pl.ds(div(3 * chip, 2), 2)]

    gu.wait()
    both = gu_send[...] + gu_recv[...]
    lane136 = lax.broadcasted_iota(jnp.int32, (FFB, 128), 1)
    active = both / (1.0 + jnp.exp(-both)) * pltpu.roll(both, 64, 1)
    act_v[c] = jnp.where(lane136 < 64, active, 0.0).astype(BF16)
    act_cp = pltpu.make_async_remote_copy(
        src_ref=act_v.at[c],
        dst_ref=act_v.at[c],
        send_sem=s4,
        recv_sem=r4,
        device_id=sibling,
        device_id_type=MESH,
    )
    act_cp.start()
    wd_cp.wait()
    pre_down.wait()
    act_cp.wait()
    for n in range(6):
        cols = slice(512 * n, 512 * n + 512)
        acc_v[:, cols] = lax.dot_general(
            act_v[0, :, 0:64], wd_v[0, :, cols], TN, preferred_element_type=F32
        ) + lax.dot_general(
            act_v[1, :, 0:64], wd_v[1, :, cols], TN, preferred_element_type=F32
        )
    wo_cp.wait()
    pre_out.wait()

    most = recv2.at[pl.ds(0, 31)]
    wait_recv(most, most, s2, r2)
    for n in range(32):
        lhs_v[2 * n : 2 * n + 2, 0:128] = recv2[n, 0].astype(F32)
        lhs_v[2 * n : 2 * n + 2, 128:256] = recv2[n, 1].astype(F32)
    lhs = lhs_v[...].astype(BF16)
    for n in range(6):
        low = slice(256 * n, 256 * n + 256)
        high = slice(1536 + 256 * n, 1536 + 256 * n + 256)
        pa = jnp.dot(lhs, wo_v[:, low], preferred_element_type=F32) + acc_v[:, low]
        pb = jnp.dot(lhs, wo_v[:, high], preferred_element_type=F32) + acc_v[:, high]
        turned = jnp.concatenate([pa, pb], axis=0).T.astype(BF16)
        for w in range(16):
            at = 256 * n + 16 * w
            zl, rest = divmod(at, 768)
            dd, e = divmod(rest, 48)
            if e == 0:
                line1[zl, dd] = turned[16 * w : 16 * w + 16]
            else:
                p1send[zl, dd, e - 16 : e, :] = turned[16 * w : 16 * w + 16]

    def push_plane(chip_to, core):
        n = 2 * chip_to + core
        pltpu.make_async_remote_copy(
            src_ref=p1send.at[:, n],
            dst_ref=recvp1.at[d16],
            send_sem=sp1,
            recv_sem=rp1,
            device_id=(s, 8 * z + chip_to, core),
            device_id_type=MESH,
        ).start()

    for dx, dy in ((2, 1), (2, 0), (1, 1), (3, 1), (1, 0), (3, 0), (0, 1)):
        chip_to = 4 * rem(y + dy, 2) + rem(x + dx, 4)
        push_plane(chip_to, 0)
        push_plane(chip_to, 1)
    push_plane(chip, 1 - c)

    def folded(part):
        half = part.shape[0] // 2
        left = lax.broadcasted_iota(jnp.int32, (half, 128), 1) < 64
        a, b = part[:half], part[half:]
        low = jnp.where(left, a, pltpu.roll(b, 64, 1)).astype(BF16)
        high = jnp.where(left, pltpu.roll(a, 64, 1), b).astype(BF16)
        return low, high

    for n in range(16):
        for zl in range(2):
            low, high = folded(line1[zl, n].astype(F32))
            zsend[zl, n] = low
            zsend[2 + zl, n] = high
    for n in range(4):
        there = 4 * c + n

        @pl.when(there != z)
        def _():
            pltpu.make_async_remote_copy(
                src_ref=zsend.at[n],
                dst_ref=zrecv.at[z],
                send_sem=sz,
                recv_sem=rz,
                device_id=(s, 8 * there + chip, c),
                device_id_type=MESH,
            ).start()

    most1 = recvp1.at[pl.ds(0, 15)]
    most2 = recvp2.at[pl.ds(0, 7)]
    mostz = zrecv.at[pl.ds(0, 7)]
    recvp1[d16] = p1send[:, d16]
    wait_recv(most1, most1, sp1, rp1)
    for cs in range(2):
        for zl in range(2):
            part = recvp1[cs, zl].astype(F32)
            for p in range(1, 8):
                part = part + recvp1[2 * p + cs, zl].astype(F32)
            low, high = folded(part)
            p2send[4 * cs + zl] = low
            p2send[4 * cs + 2 + zl] = high
    for o in (4, 3, 5, 2, 6, 1, 7):
        n = rem(z + o, 8)
        pltpu.make_async_remote_copy(
            src_ref=p2send.at[n],
            dst_ref=recvp2.at[z],
            send_sem=sp2,
            recv_sem=rp2,
            device_id=(s, 8 * n + chip, c),
            device_id_type=MESH,
        ).start()
    recvp2[z] = p2send[z]

    @pl.when(is_line)
    def _():
        zrecv[z] = zsend[rem(z, 4)]
        wait_recv(mostz, mostz, sz, rz)
        for n in range(16):
            part = zrecv[0, n].astype(F32)
            for p in range(1, 8):
                part = part + zrecv[p, n].astype(F32)
            zsum[n] = part.astype(BF16)
        for o in range(1, 16):
            n = rem(d16 + o, 16)
            pltpu.make_async_remote_copy(
                src_ref=zsum.at[n],
                dst_ref=recvz2.at[chip],
                send_sem=sz2,
                recv_sem=rz2,
                device_id=(s, 8 * z + div(n, 2), rem(n, 2)),
                device_id_type=MESH,
            ).start()
        recvz2[chip] = zsum[d16]
        seven = recvz2.at[pl.ds(0, 7)]
        wait_recv(seven, seven, sz2, rz2)

    @pl.when(jnp.logical_not(is_line))
    def _():
        wait_recv(recvz2, recvz2, sz2, rz2)

    wait_recv(most2, most2, sp2, rp2)
    last = recvp2[0].astype(F32)
    for n in range(1, 8):
        last = last + recvp2[n].astype(F32)
    line = recvz2[0].astype(F32)
    for n in range(1, 8):
        line = line + recvz2[n].astype(F32)
    result = jnp.concatenate(
        [line, pltpu.roll(line, 64, 1), last, pltpu.roll(last, 64, 1)], axis=0
    )[:, 0:64]
    out[...] = (result + res_v[pl.ds(res_off, 48), :]).astype(BF16)

    for count, when in (
        (64, jnp.logical_not(edge) & jnp.logical_not(mine)),
        (63, jnp.logical_not(edge) & mine),
        (32, edge & jnp.logical_not(mine)),
        (31, edge & mine),
    ):

        @pl.when(when)
        def _():
            part = send1.at[pl.ds(0, count)]
            wait_send(part, part, s1, r1)

    wait_send(most, most, s2, r2)
    wait_send(most1, most1, sp1, rp1)
    wait_send(most2, most2, sp2, rp2)
    for count, when in ((3, is_line), (4, jnp.logical_not(is_line))):

        @pl.when(when)
        def _():
            part = zrecv.at[pl.ds(0, count)]
            wait_send(part, part, sz, rz)

    @pl.when(is_line)
    def _():
        part = zsum.at[pl.ds(0, 15)]
        wait_send(part, part, sz2, rz2)


def body(
    hidden, gain, qkv, out_w, gate, up, down, keys, values, positions, write_slots
):
    half = THETA ** (-2.0 * np.arange(64) / HD)
    freq = jnp.asarray(np.concatenate([half, half])[None, :].astype(np.float32))
    hbm = pl.BlockSpec(memory_space=pl.ANY)
    vmem = pl.BlockSpec(memory_space=pltpu.VMEM)
    dma = pltpu.SemaphoreType.DMA
    V = pltpu.VMEM
    result = pl.pallas_call(
        kernel,
        out_shape=pltpu.VMEM((48, 64), BF16),
        in_specs=[hbm] * 12,
        out_specs=vmem,
        scratch_shapes=[
            V((64, D), BF16),
            V((96, 128), F32),
            V((128, HALF), BF16),
            V((256, NCOL), BF16),
            V((FFB, HALF), BF16),
            V((FFB, HALF), BF16),
            V((2, FFB, NCOL), BF16),
            V((2, WIN, HD), BF16),
            V((WIN, 2 * HD), BF16),
            V((64, HALF), BF16),
            V((64, 2, 128), F32),
            V((56, 2, 128), F32),
            V((2, 16, 128), F32),
            V((8, 128), F32),
            V((12, 2, 128), BF16),
            V((32, 2, 2, 128), BF16),
            V((64, 256), F32),
            V((FFB, 128), F32),
            V((FFB, 128), F32),
            V((2, FFB, 128), BF16),
            V((64, NCOL), F32),
            V((2, 16, 32, 128), BF16),
            V((16, 2, 32, 128), BF16),
            V((8, 16, 128), BF16),
            V((8, 16, 128), BF16),
            V((256, 64), F32),
            pltpu.SMEM((64,), jnp.int32),
            pltpu.SMEM((64,), jnp.int32),
            V((1, 128), F32),
            V((2, 8, WIN), F32),
            V((2, 16, 16, 128), BF16),
            V((4, 16, 8, 128), BF16),
            V((8, 16, 8, 128), BF16),
            V((16, 8, 128), BF16),
            V((8, 8, 128), BF16),
            V((32, WIN), F32),
            V((2 * HD, WIN), BF16),
            dma((17,)),
            dma, dma,
            dma((2,)), dma((2,)),
            dma, dma, dma, dma, dma, dma, dma, dma, dma, dma, dma, dma, dma, dma,
        ],
        compiler_params=pltpu.CompilerParams(
            collective_id=0, has_side_effects=True, vmem_limit_bytes=60 * 1024 * 1024
        ),
        name="layer",
    )(
        hidden,
        gain.reshape(96, 128),
        qkv.T,
        out_w,
        gate.T,
        up.T,
        down,
        keys,
        values,
        positions,
        write_slots,
        freq,
    )
    return result.T


def solution(mesh):
    side, grp, rep = mesh.axis_names
    inner = (grp, rep)
    every = (side, grp, rep)
    placed = (
        P(),
        P(),
        P(side, inner),
        P(inner, side),
        P(side, inner),
        P(side, inner),
        P(inner, side),
        P(every, None, None),
        P(every, None, None),
        P(),
        P(),
    )
    return jax.shard_map(
        body, mesh=mesh, in_specs=placed, out_specs=P(None, every), check_vma=False
    )
```
